256 devices in a mesh: row: 32 (over y_hi, z, core), col: 8 (over x, y_lo).
Axes of the slice: x: 4, y: 4 (y_hi: 2, y_lo: 2; y = y_hi * 2 + y_lo), z: 8, core: 2. Of those that a mesh axis runs over, the one named last changes fastest.
Arguments:
- hidden: bfloat16 [32768, 768], P(('row', 'col')), may hold values from -6 to 6
- projection: bfloat16 [768, 512], replicated, may hold values from -0.21875 to 0.21875
- alpha: bfloat16 [32768], P(('row', 'col')), may hold values from -6 to 6
- probe_pairs: bfloat16 [32768, 32], P(('row', 'col')), may hold values from -6 to 6
- amplitude: float32 [1], replicated, may hold values from 0.5 to 2
- length_sq: float32 [1], replicated, may hold values from 512 to 1024
Outputs:
- grad_hidden: bfloat16 [32768, 768], P(('row', 'col'))
- grad_proj: float32 [768, 512], P('row')
The draws below stay inside these ranges and needn't reach their ends.
All inputs are finite; a program needn't handle non-finite values.
Results may differ from the reference program's by a relative error of at most 0.023.
Values may be sent and summed in bfloat16 or wider, within the bound.
A program may use at most 64 MiB of HBM per device.

```python
import math
import jax
import jax.numpy as jnp
from jax import lax

HID = 768
FEAT = 512
PROBES = 16
POINTS = 32768
N_ROW = 32


def draw_hidden(key, part):
    groups = max(POINTS // 256, 2)
    centers = jax.random.normal(jax.random.fold_in(key, 13), (groups, HID), jnp.float32)
    labels = jax.random.randint(jax.random.fold_in(key, 14), (POINTS,), 0, groups)
    placed = 2.0 * jnp.take(centers, labels, axis=0)
    values = placed + jax.random.normal(jax.random.fold_in(key, 11), (POINTS, HID), jnp.float32)
    values = jnp.clip(values, -6.0, 6.0)
    return values.astype(jnp.bfloat16)


def level_of(key, extent, pieces, smallest, top_value):
    loudness, own = 1.0, jax.random.fold_in(key, 6)
    for dim, blocks in pieces:
        heights = jnp.exp(jax.random.uniform(jax.random.fold_in(own, dim), (blocks,), jnp.float32, smallest / len(pieces), top_value / len(pieces)))
        loudness = loudness * jnp.repeat(heights, extent[dim] // blocks).reshape([-1 if axis == dim else 1 for axis in range(len(extent))])
    return loudness


def bell_draw(own_key, extent, width, bound, pieces=(), held_as=jnp.bfloat16):
    entries = width * jax.random.normal(own_key, extent, jnp.float32)
    if pieces:
        entries = entries * level_of(own_key, extent, pieces, -0.22, 0.18)
    return jnp.clip(entries, -bound, bound).astype(held_as)


def setup_inputs(seed: int = 0) -> dict:
    key_of = jax.random.split(jax.random.key(seed), 7)
    return {
        "hidden": draw_hidden(jax.random.fold_in(key_of[6], 71), 0),
        "projection": bell_draw(key_of[1], (HID, FEAT), HID ** -0.5, 0.21875),
        "alpha": bell_draw(key_of[2], (POINTS,), 1.0, 6.0, ((0, 256),)),
        "probe_pairs": bell_draw(key_of[3], (POINTS, 2 * PROBES), 1.0, 6.0, ((0, 256),)),
        "amplitude": jnp.clip(jnp.exp(jax.random.uniform(key_of[4], (1,), jnp.float32, math.log(0.5), math.log(2.0))), 0.5, 2.0),
        "length_sq": jnp.clip(jnp.exp(jax.random.uniform(key_of[5], (1,), jnp.float32, math.log(512.0), math.log(1024.0))), 512.0, 1024.0),
    }


def right_of(factors, probes):
    scale = 1.0 / (4 * probes)
    return jnp.concatenate([factors[:, :1] * 0.5, factors[:, 1 + probes:] * (-scale), factors[:, 1:1 + probes] * (-scale)], axis=1)


def reference(hidden, projection, alpha, probe_pairs, amplitude, length_sq):
    feats = jnp.dot(hidden, projection, preferred_element_type=jnp.float32).astype(jnp.bfloat16)
    left = jnp.concatenate([alpha[:, None], probe_pairs], axis=1)
    probes = probe_pairs.shape[1] // 2
    right = right_of(left, probes)
    amp = amplitude[0]
    lsq = length_sq[0]
    feat_f = feats.astype(jnp.float32)
    sq_all = jnp.sum(feat_f * feat_f, axis=1)
    block = POINTS // N_ROW

    def one_block(index):
        start = (index * block).astype(jnp.int32)
        rows_feat = lax.dynamic_slice_in_dim(feats, start, block, 0)
        rows_left = lax.dynamic_slice_in_dim(left, start, block, 0)
        rows_sq = lax.dynamic_slice_in_dim(sq_all, start, block, 0)
        inner = jnp.dot(rows_feat, feats.T, preferred_element_type=jnp.float32)
        dist = rows_sq[:, None] + sq_all[None, :] - 2.0 * inner
        kern = amp * jnp.exp(-0.5 * dist / lsq)
        gmat = jnp.dot(rows_left, right.T, preferred_element_type=jnp.float32)
        weight = gmat * kern
        rowsum = jnp.sum(weight, axis=1)
        moved = jnp.dot(weight.astype(jnp.bfloat16), feats, preferred_element_type=jnp.float32)
        return moved, rowsum

    moved, rowsum = lax.map(one_block, jnp.arange(N_ROW, dtype=jnp.int32))
    moved = moved.reshape(POINTS, -1)
    rowsum = rowsum.reshape(POINTS)
    grad_feat = ((2.0 / lsq) * (moved - rowsum[:, None] * feat_f)).astype(jnp.bfloat16)
    grad_hidden = jnp.dot(grad_feat, projection.T, preferred_element_type=jnp.float32).astype(jnp.bfloat16)
    grad_proj = lax.dot_general(hidden, grad_feat, (((0,), (0,)), ((), ())), preferred_element_type=jnp.float32)
    return grad_hidden, grad_proj
```

```python
import functools
import math

import jax
import jax.numpy as jnp
from jax import lax
from jax.experimental import pallas as pl
from jax.experimental.pallas import tpu as pltpu
from jax.sharding import PartitionSpec as P

MESH = pl.DeviceIdType.MESH
NT = (((1,), (1,)), ((), ()))
TN = (((0,), (0,)), ((), ()))
BF, F32 = jnp.bfloat16, jnp.float32

NX, NY, NZ = 4, 4, 8
AUX = 128
POS = {0: 0, 4: 1, 3: 2, 5: 3, 2: 4, 6: 5, 1: 6, 7: 7}
CHUNK = 2048


def iota(shape, dim):
    return lax.broadcasted_iota(jnp.int32, shape, dim)


def aux_block(feats, alpha_row, probe, probes):
    points = feats.shape[0]
    src, lane = iota((2 * probes, AUX), 0), iota((2 * probes, AUX), 1)
    scale = 1.0 / (4 * probes)
    swapped = jnp.where(src < probes, src + probes, src - probes)
    pick = jnp.where(lane == src, 1.0, 0.0) + jnp.where(lane - 64 == swapped, -scale, 0.0)
    aux = jnp.dot(probe, pick.astype(BF), preferred_element_type=F32)
    spread = jnp.broadcast_to(alpha_row.astype(F32), (points, points))
    diag = jnp.where(iota((points, points), 0) == iota((points, points), 1), spread, 0.0)
    lane = iota((points, AUX), 1)
    put = jnp.where(lane == 2 * probes, 1.0, 0.0) + jnp.where(lane == 64 + 2 * probes, 0.5, 0.0)
    aux = aux + jnp.dot(diag.astype(BF), put.astype(BF), preferred_element_type=F32)
    f = feats.astype(F32)
    rest = jnp.sum(f * f, axis=1, keepdims=True)
    for k in range(3):
        part = rest.astype(BF).astype(F32)
        aux = jnp.where(lane == 100 + k, part, aux)
        rest = rest - part
    return aux


def kernel(
    probes,
    amp_ref,
    lsq_ref,
    hidden_ref,
    proj_ref,
    alpha_ref,
    probe_ref,
    gh_ref,
    pp_ref,
    rows,
    cols,
    left,
    bias,
    moved,
    rsum,
    sbuf,
    rplus,
    rminus,
    row_send,
    row_recv,
    col_send,
    col_recv,
    part_send,
    part_recv,
    rs_send,
    rs_recv,
):
    pts, hid = hidden_ref.shape
    feat = proj_ref.shape[1]
    width = feat + AUX
    half, quarter = pts // 2, pts // 4
    n_rows, n_cols = rows.shape[0], cols.shape[0]

    r, c = lax.axis_index("row"), lax.axis_index("col")
    k, z, y_hi = r % 2, (r // 2) % NZ, r // (2 * NZ)
    x, y_lo = c // 2, c % 2
    y = y_hi * 2 + y_lo

    def dev(dx, dy, dz, flip=0):
        xx, yy, zz = (x + dx) % NX, (y + dy) % NY, (z + dz) % NZ
        kk = (1 - k) if flip else k
        return (((yy // 2) * NZ + zz) * 2 + kk, xx * 2 + yy % 2)

    xm, xp, ym, yp = dev(-1, 0, 0), dev(1, 0, 0), dev(0, -1, 0), dev(0, 1, 0)
    zm, zp, partner = dev(0, 0, -1), dev(0, 0, 1), dev(0, 0, 0, 1)

    barrier = pltpu.get_barrier_semaphore()
    for peer in (xm, xp, ym, yp, zm, zp, partner):
        pl.semaphore_signal(barrier, inc=1, device_id=peer, device_id_type=MESH)

    feats = jnp.dot(hidden_ref[...], proj_ref[...], preferred_element_type=F32).astype(BF)
    aux = aux_block(feats, alpha_ref[...], probe_ref[...], probes).astype(BF)
    for own in (rows, cols):
        own[0:pts, 0:feat] = feats
        own[0:pts, feat:width] = aux

    pl.semaphore_wait(barrier, 7)

    sends = []

    def send(src, dst, send_sem, recv_sem, to):
        copy = pltpu.make_async_remote_copy(
            src_ref=src,
            dst_ref=dst,
            send_sem=send_sem,
            recv_sem=recv_sem,
            device_id=to,
            device_id_type=MESH,
        )
        copy.start()
        sends.append(copy)

    def arrived(dst, recv_sem):
        pltpu.make_async_remote_copy(
            src_ref=dst,
            dst_ref=dst,
            send_sem=recv_sem,
            recv_sem=recv_sem,
            device_id=partner,
            device_id_type=MESH,
        ).wait_recv()

    n_row_sends = [0]

    def row_part(d, h):
        return rows.at[pl.ds(POS[d] * pts + h * half, half), :]

    def row_send_on(d, h, to_d, to):
        i = n_row_sends[0]
        n_row_sends[0] += 1
        send(row_part(d, h), row_part(to_d, h), row_send.at[i], row_recv.at[to_d, h], to)

    def col_part(core, dx, dy, q, n):
        start = ((core * NX + dx) * NY + dy) * pts + q * quarter
        return cols.at[pl.ds(start, n * quarter), :]

    n_col_sends = [0]

    def col_send_on(dx, dy, q, n, to_dx, to_dy, to):
        i = n_col_sends[0]
        n_col_sends[0] += 1
        send(
            col_part(0, dx, dy, q, n),
            col_part(0, to_dx, to_dy, q, n),
            col_send.at[i],
            col_recv.at[to_dx, to_dy, q],
            to,
        )

    def to_partner(dx, dy, h):
        send(
            col_part(0, dx, dy, 2 * h, 2),
            col_part(1, dx, dy, 2 * h, 2),
            part_send.at[dx, dy, h],
            part_recv.at[dx, dy, h],
            partner,
        )

    def at(h, a, b):
        return (a, b) if h == 0 else (b, a)

    def first_phase(h):
        minus, plus = ((xm, xp), (ym, yp))[h]
        col_send_on(0, 0, 2 * h, 2, *at(h, 1, 0), minus)
        col_send_on(0, 0, 2 * h, 2, *at(h, 3, 0), plus)

    def first_relay(h):
        minus, plus = ((xm, xp), (ym, yp))[h]
        col_send_on(*at(h, 1, 0), 2 * h, 1, *at(h, 2, 0), minus)
        col_send_on(*at(h, 3, 0), 2 * h + 1, 1, *at(h, 2, 0), plus)

    def second_phase(h, a):
        minus, plus = ((ym, yp), (xm, xp))[h]
        col_send_on(*at(h, a, 0), 2 * h, 2, *at(h, a, 1), minus)
        col_send_on(*at(h, a, 0), 2 * h, 2, *at(h, a, 3), plus)

    def second_relay(h, a):
        minus, plus = ((ym, yp), (xm, xp))[h]
        col_send_on(*at(h, a, 1), 2 * h, 1, *at(h, a, 2), minus)
        col_send_on(*at(h, a, 3), 2 * h + 1, 1, *at(h, a, 2), plus)

    def col_wait(h, a, b):
        dx, dy = at(h, a, b)
        arrived(col_part(0, dx, dy, 2 * h, 2), col_recv.at[dx, dy, 2 * h])

    def col_wait_quarters(h, a, b):
        dx, dy = at(h, a, b)
        for q in (2 * h, 2 * h + 1):
            arrived(col_part(0, dx, dy, q, 1), col_recv.at[dx, dy, q])

    for h in (0, 1):
        first_phase(h)
        row_send_on(0, h, 1, zm)
        row_send_on(0, h, 7, zp)
    for h in (0, 1):
        second_phase(h, 0)
        to_partner(0, 0, h)
    for h in (0, 1):
        for a in (1, 3):
            col_wait(h, a, 0)
        first_relay(h)
        for a in (1, 3):
            second_phase(h, a)
        for a in (1, 3):
            to_partner(*at(h, a, 0), h)
    for h in (0, 1):
        arrived(row_part(1, h), row_recv.at[1, h])
        row_send_on(1, h, 2, zm)
        arrived(row_part(7, h), row_recv.at[7, h])
        row_send_on(7, h, 6, zp)
    for h in (0, 1):
        for b in (1, 3):
            col_wait(h, 0, b)
        second_relay(h, 0)
        for b in (1, 3):
            to_partner(*at(h, 0, b), h)
    for h in (0, 1):
        col_wait_quarters(h, 2, 0)
        second_phase(h, 2)
        to_partner(*at(h, 2, 0), h)
    for h in (0, 1):
        arrived(row_part(2, h), row_recv.at[2, h])
        row_send_on(2, h, 3, zm)
        arrived(row_part(6, h), row_recv.at[6, h])
        row_send_on(6, h, 5, zp)
    for a in (1, 3, 2):
        for h in (0, 1):
            for b in (1, 3):
                col_wait(h, a, b)
            second_relay(h, a)
            for b in (1, 3):
                to_partner(*at(h, a, b), h)
        if a == 1:
            arrived(row_part(3, 0), row_recv.at[3, 0])
            row_send_on(3, 0, 4, zm)
            arrived(row_part(5, 1), row_recv.at[5, 1])
            row_send_on(5, 1, 4, zp)
    for a in (0, 1, 3, 2):
        for h in (0, 1):
            col_wait_quarters(h, a, 2)
            to_partner(*at(h, a, 2), h)
    for d, h in ((3, 1), (5, 0), (4, 0), (4, 1)):
        arrived(row_part(d, h), row_recv.at[d, h])

    scale = math.log2(math.e) / lsq_ref[0]

    lane = iota((n_rows, AUX), 1)
    raw = rows[:, feat:width].astype(F32)
    norms = jnp.where((lane >= 100) & (lane < 103), raw, 0.0)
    bias[...] = jnp.sum(norms, axis=1, keepdims=True) * (-0.5 * scale)
    turned = pltpu.roll(raw, 64, 1)
    left[...] = jnp.where((lane >= 64) & (lane <= 64 + 2 * probes), turned, 0.0).astype(BF)
    lane16 = iota((16, AUX), 1)
    picks = jnp.where((lane16 >= 100) & (lane16 < 103), 1.0, 0.0).astype(BF)

    for core in (1,):
        for dx in range(NX):
            for dy in range(NY):
                for h in (0, 1):
                    arrived(col_part(core, dx, dy, 2 * h, 2), part_recv.at[dx, dy, h])

    def group(g):
        m = 2 * pts
        rs = pl.ds(g * m, m)

        @pl.loop(0, n_cols // CHUNK)
        def _(j):
            cs = pl.ds(pl.multiple_of(j * CHUNK, CHUNK), CHUNK)
            col_f = cols[cs, 0:feat]
            col_a = cols[cs, feat:width]
            sq = lax.dot_general(picks, col_a, NT, preferred_element_type=F32)[0:1, :]
            inner = lax.dot_general(rows[rs, 0:feat], col_f, NT, preferred_element_type=F32)
            gmat = lax.dot_general(left[rs, :], col_a, NT, preferred_element_type=F32)
            expo = inner * scale + (bias[rs, :] + sq * (-0.5 * scale))
            weight = gmat * jnp.exp2(expo)
            total = weight[:, :128]
            for t in range(1, CHUNK // 128):
                total = total + weight[:, t * 128 : (t + 1) * 128]
            term = jnp.dot(weight.astype(BF), col_f, preferred_element_type=F32)

            @pl.when(j == 0)
            def _():
                rsum[...] = total
                moved[rs, :] = term

            @pl.when(j > 0)
            def _():
                rsum[...] += total
                moved[rs, :] += term

        rowsum = jnp.sum(rsum[...], axis=1, keepdims=True)
        moved[rs, :] = moved[rs, :] - rowsum * rows[rs, 0:feat].astype(F32)

    n_rs = [0]

    def pass_on(d, h, step, to, dst, arrival=None):
        rs = pl.ds(POS[d] * pts + h * half, half)
        hs = pl.ds(h * half, half)
        value = moved[rs, :]
        way = 0 if dst is rplus else 1
        if arrival is not None:
            ref = dst.at[arrival, hs, :]
            arrived(ref, rs_recv.at[way, arrival, h])
            value = value + dst[arrival, hs, :].astype(F32)
        sbuf[rs, :] = value.astype(BF)
        i = n_rs[0]
        n_rs[0] += 1
        send(sbuf.at[rs, :], dst.at[step, hs, :], rs_send.at[i], rs_recv.at[way, step, h], to)

    group(0)
    pass_on(4, 0, 0, zp, rplus)
    pass_on(4, 1, 0, zm, rminus)
    group(1)
    pass_on(3, 1, 1, zp, rplus)
    pass_on(5, 0, 1, zm, rminus)
    pass_on(3, 0, 1, zp, rplus, 0)
    pass_on(5, 1, 1, zm, rminus, 0)
    group(2)
    for h in (0, 1):
        pass_on(2, h, 2, zp, rplus, 1)
        pass_on(6, h, 2, zm, rminus, 1)
    group(3)
    for h in (0, 1):
        pass_on(1, h, 3, zp, rplus, 2)
        pass_on(7, h, 3, zm, rminus, 2)
    for h in (0, 1):
        hs = pl.ds(h * half, half)
        arrived(rplus.at[3, hs, :], rs_recv.at[0, 3, h])
        arrived(rminus.at[3, hs, :], rs_recv.at[1, 3, h])
    total = moved[0:pts, :] + rplus[3].astype(F32) + rminus[3].astype(F32)
    grad = (total * (2.0 * amp_ref[0] / lsq_ref[0])).astype(BF)
    gh_ref[...] = lax.dot_general(grad, proj_ref[...], NT, preferred_element_type=F32).astype(BF)
    pp_ref[...] = lax.dot_general(
        hidden_ref[...], grad, TN, preferred_element_type=F32
    ).astype(BF)
    for copy in sends:
        copy.wait_send()


def fused(hidden, projection, alpha, probe_pairs, amplitude, length_sq):
    pts, hid = hidden.shape
    feat = projection.shape[1]
    probes = probe_pairs.shape[1] // 2
    width = feat + AUX
    n_rows, n_cols = NZ * pts, 2 * NX * NY * pts
    half = pts // 2
    vmem = pl.BlockSpec(memory_space=pltpu.VMEM)
    smem = pl.BlockSpec(memory_space=pltpu.SMEM)
    dma = pltpu.SemaphoreType.DMA
    return pl.pallas_call(
        functools.partial(kernel, probes),
        out_shape=(
            jax.ShapeDtypeStruct((pts, hid), BF),
            jax.ShapeDtypeStruct((hid, feat), BF),
        ),
        in_specs=[smem, smem, vmem, vmem, vmem, vmem],
        out_specs=(vmem, vmem),
        scratch_shapes=[
            pltpu.VMEM((n_rows, width), BF),
            pltpu.VMEM((n_cols, width), BF),
            pltpu.VMEM((n_rows, AUX), BF),
            pltpu.VMEM((n_rows, 1), F32),
            pltpu.VMEM((n_rows, feat), F32),
            pltpu.VMEM((2 * pts, 128), F32),
            pltpu.VMEM((n_rows, feat), BF),
            pltpu.VMEM((4, pts, feat), BF),
            pltpu.VMEM((4, pts, feat), BF),
            dma((14,)),
            dma((NZ, 2)),
            dma((40,)),
            dma((NX, NY, 4)),
            dma((NX, NY, 2)),
            dma((NX, NY, 2)),
            dma((14,)),
            dma((2, 4, 2)),
        ],
        compiler_params=pltpu.CompilerParams(
            collective_id=0, has_side_effects=True, vmem_limit_bytes=56 << 20
        ),
        name="fused",
    )(amplitude, length_sq, hidden, projection, alpha[None, :], probe_pairs)


def per_device(hidden, projection, alpha, probe_pairs, amplitude, length_sq):
    grad_hidden, partial = fused(hidden, projection, alpha, probe_pairs, amplitude, length_sq)
    size = lax.axis_size("row")
    blocks = partial.reshape(size, partial.shape[0] // size, partial.shape[1])
    blocks = lax.all_to_all(blocks, "row", split_axis=0, concat_axis=0, tiled=True)
    share = blocks.astype(F32).sum(axis=0).astype(BF)
    size = lax.axis_size("col")
    every = lax.all_to_all(jnp.broadcast_to(share[None], (size, *share.shape)), "col", 0, 0, tiled=True)
    return grad_hidden, jnp.sum(every.astype(F32), axis=0)


def solution(mesh):
    placed = (P(("row", "col"), None), P(), P(("row", "col")), P(("row", "col"), None), P(), P())
    return jax.shard_map(
        per_device,
        mesh=mesh,
        in_specs=placed,
        out_specs=(P(("row", "col"), None), P("row", None)),
        check_vma=False,
    )
```

```python
import functools
import math

import jax
import jax.numpy as jnp
from jax import lax
from jax.experimental import pallas as pl
from jax.experimental.pallas import tpu as pltpu
from jax.sharding import PartitionSpec as P

MESH = pl.DeviceIdType.MESH
NT = (((1,), (1,)), ((), ()))
TN = (((0,), (0,)), ((), ()))
BF, F32 = jnp.bfloat16, jnp.float32

NX, NY, NZ = 4, 4, 8
AUX = 128
POS = {0: 0, 4: 1, 3: 2, 5: 3, 2: 4, 6: 5, 1: 6, 7: 7}
CHUNK = 2048


def iota(shape, dim):
    return lax.broadcasted_iota(jnp.int32, shape, dim)


def aux_block(feats, alpha_row, probe_t, probes):
    points = feats.shape[0]
    src, lane = iota((2 * probes, AUX), 0), iota((2 * probes, AUX), 1)
    scale = 1.0 / (4 * probes)
    swapped = jnp.where(src < probes, src + probes, src - probes)
    pick = jnp.where(lane == src, 1.0, 0.0) + jnp.where(lane - 64 == swapped, -scale, 0.0)
    aux = lax.dot_general(probe_t, pick.astype(BF), TN, preferred_element_type=F32)
    spread = jnp.broadcast_to(alpha_row.astype(F32), (points, points))
    diag = jnp.where(iota((points, points), 0) == iota((points, points), 1), spread, 0.0)
    lane = iota((points, AUX), 1)
    put = jnp.where(lane == 2 * probes, 1.0, 0.0) + jnp.where(lane == 64 + 2 * probes, 0.5, 0.0)
    aux = aux + jnp.dot(diag.astype(BF), put.astype(BF), preferred_element_type=F32)
    f = feats.astype(F32)
    rest = jnp.sum(f * f, axis=1, keepdims=True)
    for k in range(3):
        part = rest.astype(BF).astype(F32)
        aux = jnp.where(lane == 100 + k, part, aux)
        rest = rest - part
    return aux


def kernel(
    probes,
    amp_ref,
    lsq_ref,
    hidden_ref,
    proj_ref,
    alpha_ref,
    probe_ref,
    gh_ref,
    gp_ref,
    rows,
    cols,
    left,
    bias,
    moved,
    rsum,
    sbuf,
    rplus,
    rminus,
    row_send,
    row_recv,
    col_send,
    col_recv,
    part_send,
    part_recv,
    rs_send,
    rs_recv,
    other_hid,
    gbuf,
    pbuf,
    prec,
    zbuf,
    zrec,
    fbuf,
    frec,
    pair_send,
    pair_recv,
    p_send,
    p_recv,
    z_send,
    z_recv,
    f_send,
    f_recv,
):
    pts, hid = hidden_ref.shape
    feat = proj_ref.shape[1]
    width = feat + AUX
    half, quarter = pts // 2, pts // 4
    n_rows, n_cols = rows.shape[0], cols.shape[0]

    r, c = lax.axis_index("row"), lax.axis_index("col")
    k, z, y_hi = r % 2, (r // 2) % NZ, r // (2 * NZ)
    x, y_lo = c // 2, c % 2
    y = y_hi * 2 + y_lo

    def dev(dx, dy, dz, flip=0):
        xx, yy, zz = (x + dx) % NX, (y + dy) % NY, (z + dz) % NZ
        kk = (1 - k) if flip else k
        return (((yy // 2) * NZ + zz) * 2 + kk, xx * 2 + yy % 2)

    xm, xp, ym, yp = dev(-1, 0, 0), dev(1, 0, 0), dev(0, -1, 0), dev(0, 1, 0)
    zm, zp, partner = dev(0, 0, -1), dev(0, 0, 1), dev(0, 0, 0, 1)

    barrier = pltpu.get_barrier_semaphore()
    for peer in (xm, xp, ym, yp, zm, zp, partner):
        pl.semaphore_signal(barrier, inc=1, device_id=peer, device_id_type=MESH)

    feats = jnp.dot(hidden_ref[...], proj_ref[...], preferred_element_type=F32).astype(BF)
    aux = aux_block(feats, alpha_ref[...], probe_ref[...], probes).astype(BF)
    for own in (rows, cols):
        own[0:pts, 0:feat] = feats
        own[0:pts, feat:width] = aux

    pl.semaphore_wait(barrier, 7)

    sends = []

    def send(src, dst, send_sem, recv_sem, to):
        copy = pltpu.make_async_remote_copy(
            src_ref=src,
            dst_ref=dst,
            send_sem=send_sem,
            recv_sem=recv_sem,
            device_id=to,
            device_id_type=MESH,
        )
        copy.start()
        sends.append(copy)

    def arrived(dst, recv_sem):
        pltpu.make_async_remote_copy(
            src_ref=dst,
            dst_ref=dst,
            send_sem=recv_sem,
            recv_sem=recv_sem,
            device_id=partner,
            device_id_type=MESH,
        ).wait_recv()

    n_row_sends = [0]

    def row_part(d, h):
        return rows.at[pl.ds(POS[d] * pts + h * half, half), :]

    def row_send_on(d, h, to_d, to):
        i = n_row_sends[0]
        n_row_sends[0] += 1
        send(row_part(d, h), row_part(to_d, h), row_send.at[i], row_recv.at[to_d, h], to)

    def col_part(core, dx, dy, q, n):
        start = ((core * NX + dx) * NY + dy) * pts + q * quarter
        return cols.at[pl.ds(start, n * quarter), :]

    n_col_sends = [0]

    def col_send_on(dx, dy, q, n, to_dx, to_dy, to):
        i = n_col_sends[0]
        n_col_sends[0] += 1
        send(
            col_part(0, dx, dy, q, n),
            col_part(0, to_dx, to_dy, q, n),
            col_send.at[i],
            col_recv.at[to_dx, to_dy, q],
            to,
        )

    def to_partner(dx, dy, h):
        send(
            col_part(0, dx, dy, 2 * h, 2),
            col_part(1, dx, dy, 2 * h, 2),
            part_send.at[dx, dy, h],
            part_recv.at[dx, dy, h],
            partner,
        )

    def at(h, a, b):
        return (a, b) if h == 0 else (b, a)

    def first_phase(h):
        minus, plus = ((xm, xp), (ym, yp))[h]
        col_send_on(0, 0, 2 * h, 2, *at(h, 1, 0), minus)
        col_send_on(0, 0, 2 * h, 2, *at(h, 3, 0), plus)

    def first_relay(h):
        minus, plus = ((xm, xp), (ym, yp))[h]
        col_send_on(*at(h, 1, 0), 2 * h, 1, *at(h, 2, 0), minus)
        col_send_on(*at(h, 3, 0), 2 * h + 1, 1, *at(h, 2, 0), plus)

    def second_phase(h, a):
        minus, plus = ((ym, yp), (xm, xp))[h]
        col_send_on(*at(h, a, 0), 2 * h, 2, *at(h, a, 1), minus)
        col_send_on(*at(h, a, 0), 2 * h, 2, *at(h, a, 3), plus)

    def second_relay(h, a):
        minus, plus = ((ym, yp), (xm, xp))[h]
        col_send_on(*at(h, a, 1), 2 * h, 1, *at(h, a, 2), minus)
        col_send_on(*at(h, a, 3), 2 * h + 1, 1, *at(h, a, 2), plus)

    def col_wait(h, a, b):
        dx, dy = at(h, a, b)
        arrived(col_part(0, dx, dy, 2 * h, 2), col_recv.at[dx, dy, 2 * h])

    def col_wait_quarters(h, a, b):
        dx, dy = at(h, a, b)
        for q in (2 * h, 2 * h + 1):
            arrived(col_part(0, dx, dy, q, 1), col_recv.at[dx, dy, q])

    send(hidden_ref, other_hid, pair_send.at[0], pair_recv.at[0], partner)
    for h in (0, 1):
        first_phase(h)
        row_send_on(0, h, 1, zm)
        row_send_on(0, h, 7, zp)
    for h in (0, 1):
        second_phase(h, 0)
        to_partner(0, 0, h)
    for h in (0, 1):
        for a in (1, 3):
            col_wait(h, a, 0)
        first_relay(h)
    for h in (0, 1):
        for a in (1, 3):
            second_phase(h, a)
        for a in (1, 3):
            to_partner(*at(h, a, 0), h)
    for h in (0, 1):
        arrived(row_part(1, h), row_recv.at[1, h])
        row_send_on(1, h, 2, zm)
        arrived(row_part(7, h), row_recv.at[7, h])
        row_send_on(7, h, 6, zp)
    for h in (0, 1):
        for b in (1, 3):
            col_wait(h, 0, b)
        second_relay(h, 0)
        for b in (1, 3):
            to_partner(*at(h, 0, b), h)
    for h in (0, 1):
        col_wait_quarters(h, 2, 0)
        second_phase(h, 2)
        to_partner(*at(h, 2, 0), h)
    for h in (0, 1):
        arrived(row_part(2, h), row_recv.at[2, h])
        row_send_on(2, h, 3, zm)
        arrived(row_part(6, h), row_recv.at[6, h])
        row_send_on(6, h, 5, zp)
    for a in (1, 3, 2):
        for h in (0, 1):
            for b in (1, 3):
                col_wait(h, a, b)
            second_relay(h, a)
            for b in (1, 3):
                to_partner(*at(h, a, b), h)
        if a == 1:
            arrived(row_part(3, 0), row_recv.at[3, 0])
            row_send_on(3, 0, 4, zm)
            arrived(row_part(5, 1), row_recv.at[5, 1])
            row_send_on(5, 1, 4, zp)
    for a in (0, 1, 3, 2):
        for h in (0, 1):
            col_wait_quarters(h, a, 2)
            to_partner(*at(h, a, 2), h)
    for d, h in ((3, 1), (5, 0), (4, 0), (4, 1)):
        arrived(row_part(d, h), row_recv.at[d, h])

    scale = math.log2(math.e) / lsq_ref[0]

    lane = iota((n_rows, AUX), 1)
    raw = rows[:, feat:width].astype(F32)
    norms = jnp.where((lane >= 100) & (lane < 103), raw, 0.0)
    bias[...] = jnp.sum(norms, axis=1, keepdims=True) * (-0.5 * scale)
    turned = pltpu.roll(raw, 64, 1)
    left[...] = jnp.where((lane >= 64) & (lane <= 64 + 2 * probes), turned, 0.0).astype(BF)
    lane16 = iota((16, AUX), 1)
    picks = jnp.where((lane16 >= 100) & (lane16 < 103), 1.0, 0.0).astype(BF)

    for core in (1,):
        for dx in range(NX):
            for dy in range(NY):
                for h in (0, 1):
                    arrived(col_part(core, dx, dy, 2 * h, 2), part_recv.at[dx, dy, h])

    def group(g):
        m = 2 * pts
        rs = pl.ds(g * m, m)

        @pl.loop(0, n_cols // CHUNK)
        def _(j):
            cs = pl.ds(pl.multiple_of(j * CHUNK, CHUNK), CHUNK)
            col_f = cols[cs, 0:feat]
            col_a = cols[cs, feat:width]
            sq = lax.dot_general(picks, col_a, NT, preferred_element_type=F32)[0:1, :]
            inner = lax.dot_general(rows[rs, 0:feat], col_f, NT, preferred_element_type=F32)
            gmat = lax.dot_general(left[rs, :], col_a, NT, preferred_element_type=F32)
            expo = inner * scale + (bias[rs, :] + sq * (-0.5 * scale))
            weight = gmat * jnp.exp2(expo)
            total = weight[:, :128]
            for t in range(1, CHUNK // 128):
                total = total + weight[:, t * 128 : (t + 1) * 128]
            term = jnp.dot(weight.astype(BF), col_f, preferred_element_type=F32)

            @pl.when(j == 0)
            def _():
                rsum[...] = total
                moved[rs, :] = term

            @pl.when(j > 0)
            def _():
                rsum[...] += total
                moved[rs, :] += term

        rowsum = jnp.sum(rsum[...], axis=1, keepdims=True)
        moved[rs, :] = moved[rs, :] - rowsum * rows[rs, 0:feat].astype(F32)

    n_rs = [0]

    def pass_on(d, h, step, to, dst, arrival=None):
        rs = pl.ds(POS[d] * pts + h * half, half)
        hs = pl.ds(h * half, half)
        value = moved[rs, :]
        way = 0 if dst is rplus else 1
        if arrival is not None:
            ref = dst.at[arrival, hs, :]
            arrived(ref, rs_recv.at[way, arrival, h])
            value = value + dst[arrival, hs, :].astype(F32)
        sbuf[rs, :] = value.astype(BF)
        i = n_rs[0]
        n_rs[0] += 1
        send(sbuf.at[rs, :], dst.at[step, hs, :], rs_send.at[i], rs_recv.at[way, step, h], to)

    group(0)
    pass_on(4, 0, 0, zp, rplus)
    pass_on(4, 1, 0, zm, rminus)
    group(1)
    pass_on(3, 1, 1, zp, rplus)
    pass_on(5, 0, 1, zm, rminus)
    pass_on(3, 0, 1, zp, rplus, 0)
    pass_on(5, 1, 1, zm, rminus, 0)
    group(2)
    for h in (0, 1):
        pass_on(2, h, 2, zp, rplus, 1)
        pass_on(6, h, 2, zm, rminus, 1)
    group(3)
    for h in (0, 1):
        pass_on(1, h, 3, zp, rplus, 2)
        pass_on(7, h, 3, zm, rminus, 2)
    for h in (0, 1):
        hs = pl.ds(h * half, half)
        arrived(rplus.at[3, hs, :], rs_recv.at[0, 3, h])
        arrived(rminus.at[3, hs, :], rs_recv.at[1, 3, h])
    total = moved[0:pts, :] + rplus[3].astype(F32) + rminus[3].astype(F32)
    grad = (total * (2.0 * amp_ref[0] / lsq_ref[0])).astype(BF)
    gbuf[0] = grad

    proj_own = lax.dot_general(hidden_ref[...], grad, TN, preferred_element_type=F32)
    send(gbuf.at[0], gbuf.at[1], pair_send.at[1], pair_recv.at[1], partner)
    arrived(other_hid, pair_recv.at[0])
    arrived(gbuf.at[1], pair_recv.at[1])
    terms = proj_own + lax.dot_general(other_hid[...], gbuf[1], TN, preferred_element_type=F32)
    size = hid // (4 * NZ)
    for hi in range(2):
        for zz in range(NZ):
            for core in range(2):
                start = ((hi * NZ + zz) * 2 + core) * size
                pbuf[hi, core, zz] = terms[start : start + size, :].astype(BF)

    zs = pl.ds(k * (NZ // 2), NZ // 2)

    def portion(xx, yy):
        return yy // 2, yy % 2, zs, slice(None), pl.ds(pl.multiple_of(xx * 128, 128), 128)

    for dx in range(NX):
        for dy in range(NY):
            if dx or dy:
                to = ((NX - dx) % NX, (NY - dy) % NY)
                send(
                    pbuf.at[portion((x + dx) % NX, (y + dy) % NY)],
                    prec.at[to[0], to[1]],
                    p_send.at[dx, dy],
                    p_recv.at[to[0], to[1]],
                    dev(dx, dy, 0),
                )
    gh_ref[...] = lax.dot_general(grad, proj_ref[...], NT, preferred_element_type=F32).astype(BF)
    share = pbuf[portion(x, y)].astype(F32)
    for dx in range(NX):
        for dy in range(NY):
            if dx or dy:
                arrived(prec.at[dx, dy], p_recv.at[dx, dy])
                share = share + prec[dx, dy].astype(F32)
    zbuf[...] = share.astype(BF)

    gathers = k == z // (NZ // 2)
    later = []

    def send_if(cond, src, dst, send_sem, recv_sem, to):
        copy = pltpu.make_async_remote_copy(
            src_ref=src,
            dst_ref=dst,
            send_sem=send_sem,
            recv_sem=recv_sem,
            device_id=to,
            device_id_type=MESH,
        )

        @pl.when(cond)
        def _():
            copy.start()

        later.append((cond, copy))

    for dz in range(1, NZ):
        zz = (z + dz) % NZ
        send_if(
            zz // (NZ // 2) == k,
            zbuf.at[zz % (NZ // 2)],
            zrec.at[NZ - dz],
            z_send.at[dz],
            z_recv.at[NZ - dz],
            dev(0, 0, dz),
        )

    @pl.when(gathers)
    def _():
        total = zbuf[z % (NZ // 2)].astype(F32)
        for dz in range(1, NZ):
            arrived(zrec.at[dz], z_recv.at[dz])
            total = total + zrec[dz].astype(F32)
        fbuf[...] = total

    mine = y_lo == k
    for dx in range(NX):
        for flip in range(2):
            xx, yy = (x + dx) % NX, y_hi * 2 + (y_lo if flip == 0 else 1 - y_lo)
            to = ((y_hi * NZ + z) * 2 + y_lo, xx * 2 + yy % 2)
            cond = gathers if dx or flip else gathers & jnp.logical_not(mine)
            slot = (NX - dx) % NX
            send_if(cond, fbuf, frec.at[slot], f_send.at[dx, flip], f_recv.at[slot], to)

    @pl.when(gathers & mine)
    def _():
        frec[0] = fbuf[...]

    for dx in range(NX):
        if dx == 0:

            @pl.when(jnp.logical_not(gathers & mine))
            def _():
                arrived(frec.at[0], f_recv.at[0])

        else:
            arrived(frec.at[dx], f_recv.at[dx])
        gp_ref[:, pl.ds(pl.multiple_of((x + dx) % NX * 128, 128), 128)] = frec[dx]

    for copy in sends:
        copy.wait_send()
    for cond, copy in later:

        @pl.when(cond)
        def _():
            copy.wait_send()


def fused(hidden, projection, alpha, probe_pairs, amplitude, length_sq):
    pts, hid = hidden.shape
    feat = projection.shape[1]
    probes = probe_pairs.shape[1] // 2
    width = feat + AUX
    n_rows, n_cols = NZ * pts, 2 * NX * NY * pts
    half = pts // 2
    vmem = pl.BlockSpec(memory_space=pltpu.VMEM)
    smem = pl.BlockSpec(memory_space=pltpu.SMEM)
    dma = pltpu.SemaphoreType.DMA
    return pl.pallas_call(
        functools.partial(kernel, probes),
        out_shape=(
            jax.ShapeDtypeStruct((pts, hid), BF),
            jax.ShapeDtypeStruct((hid // (4 * NZ), feat), F32),
        ),
        in_specs=[smem, smem, vmem, vmem, vmem, vmem],
        out_specs=(vmem, vmem),
        scratch_shapes=[
            pltpu.VMEM((n_rows, width), BF),
            pltpu.VMEM((n_cols, width), BF),
            pltpu.VMEM((n_rows, AUX), BF),
            pltpu.VMEM((n_rows, 1), F32),
            pltpu.VMEM((n_rows, feat), F32),
            pltpu.VMEM((2 * pts, 128), F32),
            pltpu.VMEM((n_rows, feat), BF),
            pltpu.VMEM((4, pts, feat), BF),
            pltpu.VMEM((4, pts, feat), BF),
            dma((14,)),
            dma((NZ, 2)),
            dma((40,)),
            dma((NX, NY, 4)),
            dma((NX, NY, 2)),
            dma((NX, NY, 2)),
            dma((14,)),
            dma((2, 4, 2)),
            pltpu.VMEM((pts, hid), BF),
            pltpu.VMEM((2, pts, feat), BF),
            pltpu.VMEM((2, 2, NZ, hid // (4 * NZ), feat), BF),
            pltpu.VMEM((NX, NY, NZ // 2, hid // (4 * NZ), 128), BF),
            pltpu.VMEM((NZ // 2, hid // (4 * NZ), 128), BF),
            pltpu.VMEM((NZ, hid // (4 * NZ), 128), BF),
            pltpu.VMEM((hid // (4 * NZ), 128), F32),
            pltpu.VMEM((NX, hid // (4 * NZ), 128), F32),
            dma((2,)),
            dma((2,)),
            dma((NX, NY)),
            dma((NX, NY)),
            dma((NZ,)),
            dma((NZ,)),
            dma((NX, 2)),
            dma((NX,)),
        ],
        compiler_params=pltpu.CompilerParams(
            collective_id=0, has_side_effects=True, vmem_limit_bytes=56 << 20
        ),
        name="fused",
    )(amplitude, length_sq, hidden, projection, alpha[None, :], probe_pairs.T)


def per_device(hidden, projection, alpha, probe_pairs, amplitude, length_sq):
    return fused(hidden, projection, alpha, probe_pairs, amplitude, length_sq)


def solution(mesh):
    placed = (P(("row", "col"), None), P(), P(("row", "col")), P(("row", "col"), None), P(), P())
    return jax.shard_map(
        per_device,
        mesh=mesh,
        in_specs=placed,
        out_specs=(P(("row", "col"), None), P("row", None)),
        check_vma=False,
    )
```

```python
import functools
import math

import jax
import jax.numpy as jnp
from jax import lax
from jax.experimental import pallas as pl
from jax.experimental.pallas import tpu as pltpu
from jax.sharding import PartitionSpec as P

MESH = pl.DeviceIdType.MESH
NT = (((1,), (1,)), ((), ()))
TN = (((0,), (0,)), ((), ()))
BF, F32 = jnp.bfloat16, jnp.float32

NX, NY, NZ = 4, 4, 8
AUX = 128
POS = {0: 0, 4: 1, 3: 2, 5: 3, 2: 4, 6: 5, 1: 6, 7: 7}
GROUPS = 4
CHUNK = 1024
PARTS = 4
SLOTS = [
    (0, 0, 0), (1, 0, 0), (0, 0, 1), (0, 0, 3), (0, 1, 0), (0, 3, 0), (1, 0, 1), (1, 0, 3),
    (1, 1, 0), (1, 3, 0), (0, 1, 1), (0, 1, 3), (0, 3, 1), (0, 3, 3), (1, 1, 1), (0, 0, 2),
    (0, 2, 0), (1, 1, 3), (1, 3, 1), (1, 3, 3), (1, 0, 2), (1, 2, 0), (0, 1, 2), (0, 2, 1),
    (0, 2, 3), (0, 3, 2), (1, 1, 2), (1, 2, 1), (1, 2, 3), (1, 3, 2), (0, 2, 2), (1, 2, 2),
]
PLAN = [
    ("r", 0, 0, 1, 0), ("r", 0, 0, 7, 1), ("r", 0, 1, 1, 0), ("r", 0, 1, 7, 1), ("r", 0, 2, 1, 0), ("r", 0, 2, 7, 1),
    ("r", 0, 3, 1, 0), ("r", 0, 3, 7, 1), ("c", 0, 0, 0, 1, 0, 0), ("c", 0, 0, 1, 1, 0, 0), ("c", 0, 0, 2, 0, 1, 2),
    ("c", 0, 0, 3, 0, 1, 2), ("c", 0, 0, 0, 3, 0, 1), ("c", 0, 0, 1, 3, 0, 1), ("c", 0, 0, 2, 0, 3, 3),
    ("c", 0, 0, 3, 0, 3, 3), ("c", 0, 0, 0, 0, 1, 2), ("c", 0, 0, 1, 0, 1, 2), ("c", 0, 0, 2, 1, 0, 0),
    ("c", 0, 0, 3, 1, 0, 0), ("c", 0, 0, 0, 0, 3, 3), ("c", 0, 0, 1, 0, 3, 3), ("c", 0, 0, 2, 3, 0, 1),
    ("c", 0, 0, 3, 3, 0, 1), ("p", 0, 0, 0), ("p", 0, 0, 1), ("wp", 0, 0, 0), ("wp", 0, 0, 1), ("wc", 0, 1, 2),
    ("c", 0, 1, 2, 0, 2, 2), ("c", 0, 1, 2, 1, 1, 0), ("c", 0, 1, 2, 3, 1, 1), ("wc", 0, 3, 2),
    ("c", 0, 3, 2, 1, 3, 0), ("c", 0, 3, 2, 3, 3, 1), ("wc", 1, 0, 0), ("c", 1, 0, 0, 2, 0, 0),
    ("c", 1, 0, 0, 1, 1, 2), ("c", 1, 0, 0, 1, 3, 3), ("wc", 3, 0, 0), ("c", 3, 0, 0, 3, 1, 2),
    ("c", 3, 0, 0, 3, 3, 3), ("wr", 1, 0), ("r", 1, 0, 2, 0), ("wr", 7, 0), ("r", 7, 0, 6, 1), ("wc", 0, 1, 3),
    ("c", 0, 1, 3, 1, 1, 0), ("c", 0, 1, 3, 3, 1, 1), ("p", 0, 1, 1), ("wc", 0, 3, 3), ("c", 0, 3, 3, 0, 2, 3),
    ("c", 0, 3, 3, 1, 3, 0), ("c", 0, 3, 3, 3, 3, 1), ("p", 0, 3, 1), ("wc", 1, 0, 1), ("c", 1, 0, 1, 1, 1, 2),
    ("c", 1, 0, 1, 1, 3, 3), ("p", 1, 0, 0), ("wc", 3, 0, 1), ("c", 3, 0, 1, 2, 0, 1), ("c", 3, 0, 1, 3, 1, 2),
    ("c", 3, 0, 1, 3, 3, 3), ("p", 3, 0, 0), ("wr", 1, 1), ("r", 1, 1, 2, 0), ("wr", 7, 1), ("r", 7, 1, 6, 1),
    ("wc", 0, 1, 0), ("c", 0, 1, 0, 0, 2, 2), ("wc", 0, 3, 0), ("wc", 1, 0, 2), ("c", 1, 0, 2, 2, 0, 0),
    ("wc", 3, 0, 2), ("wp", 0, 1, 1), ("wp", 0, 3, 1), ("wc", 0, 1, 1), ("p", 0, 1, 0), ("wc", 0, 3, 1),
    ("c", 0, 3, 1, 0, 2, 3), ("p", 0, 3, 0), ("wc", 1, 0, 3), ("p", 1, 0, 1), ("wc", 3, 0, 3),
    ("c", 3, 0, 3, 2, 0, 1), ("p", 3, 0, 1), ("wp", 1, 0, 0), ("wr", 1, 2), ("r", 1, 2, 2, 0), ("wr", 7, 2),
    ("r", 7, 2, 6, 1), ("wp", 3, 0, 0), ("wc", 0, 2, 2), ("c", 0, 2, 2, 1, 2, 0), ("c", 0, 2, 2, 3, 2, 1),
    ("wc", 1, 1, 2), ("c", 1, 1, 2, 2, 1, 0), ("wc", 1, 3, 0), ("wc", 3, 1, 2), ("wp", 0, 1, 0), ("wr", 1, 3),
    ("r", 1, 3, 2, 0), ("wr", 7, 3), ("r", 7, 3, 6, 1), ("wp", 0, 3, 0), ("G", 3), ("g", 3, 0), ("wr", 2, 0),
    ("r", 2, 0, 3, 0), ("wr", 6, 0), ("r", 6, 0, 5, 1), ("wc", 0, 2, 3), ("c", 0, 2, 3, 1, 2, 0),
    ("c", 0, 2, 3, 3, 2, 1), ("p", 0, 2, 1), ("wc", 2, 0, 0), ("c", 2, 0, 0, 2, 1, 2), ("c", 2, 0, 0, 2, 3, 3),
    ("wc", 1, 1, 0), ("c", 1, 1, 0, 1, 2, 2), ("wc", 1, 3, 2), ("c", 1, 3, 2, 2, 3, 0), ("wc", 3, 3, 0),
    ("wc", 3, 3, 2), ("wc", 3, 1, 0), ("c", 3, 1, 0, 3, 2, 2), ("wc", 3, 1, 3), ("c", 3, 1, 3, 2, 1, 1),
    ("p", 3, 1, 1), ("wp", 1, 0, 1), ("wc", 1, 1, 1), ("p", 1, 1, 0), ("wc", 1, 1, 3), ("p", 1, 1, 1),
    ("wc", 1, 3, 1), ("c", 1, 3, 1, 1, 2, 3), ("p", 1, 3, 0), ("wc", 3, 3, 3), ("c", 3, 3, 3, 2, 3, 1),
    ("p", 3, 3, 1), ("wp", 3, 0, 1), ("wr", 2, 1), ("r", 2, 1, 3, 0), ("wr", 6, 1), ("r", 6, 1, 5, 1),
    ("wc", 2, 0, 1), ("c", 2, 0, 1, 2, 1, 2), ("c", 2, 0, 1, 2, 3, 3), ("p", 2, 0, 0), ("wc", 1, 3, 3),
    ("p", 1, 3, 1), ("wc", 3, 1, 1), ("p", 3, 1, 0), ("wc", 3, 3, 1), ("c", 3, 3, 1, 3, 2, 3), ("p", 3, 3, 0),
    ("wp", 0, 2, 1), ("wp", 3, 1, 1), ("wr", 2, 2), ("r", 2, 2, 3, 0), ("wr", 6, 2), ("r", 6, 2, 5, 1),
    ("wp", 1, 1, 0), ("wc", 0, 2, 0), ("wc", 0, 2, 1), ("p", 0, 2, 0), ("wc", 2, 0, 2), ("wc", 2, 0, 3),
    ("p", 2, 0, 1), ("wp", 1, 1, 1), ("g", 3, 1), ("wr", 2, 3), ("r", 2, 3, 3, 0), ("wr", 6, 3), ("r", 6, 3, 5, 1),
    ("wc", 1, 2, 2), ("c", 1, 2, 2, 2, 2, 0), ("wc", 3, 2, 2), ("wc", 2, 1, 0), ("c", 2, 1, 0, 2, 2, 2),
    ("wc", 2, 3, 0), ("wp", 1, 3, 0), ("wp", 3, 3, 1), ("wp", 2, 0, 0), ("wp", 1, 3, 1), ("wp", 3, 1, 0), ("G", 2),
    ("g", 2, 0), ("wr", 3, 0), ("r", 3, 0, 4, 0), ("wr", 5, 0), ("wc", 3, 2, 3), ("c", 3, 2, 3, 2, 2, 1),
    ("p", 3, 2, 1), ("wc", 1, 2, 3), ("p", 1, 2, 1), ("wc", 2, 3, 1), ("c", 2, 3, 1, 2, 2, 3), ("p", 2, 3, 0),
    ("wc", 2, 1, 2), ("wr", 3, 1), ("r", 3, 1, 4, 0), ("wr", 5, 1), ("wc", 1, 2, 0), ("wc", 1, 2, 1), ("p", 1, 2, 0),
    ("wc", 2, 1, 3), ("p", 2, 1, 1), ("wc", 3, 2, 0), ("wc", 2, 3, 2), ("wc", 2, 3, 3), ("p", 2, 3, 1),
    ("wp", 3, 3, 0), ("wp", 0, 2, 0), ("wp", 2, 0, 1), ("g", 2, 1), ("wr", 3, 2), ("wr", 5, 2), ("r", 5, 2, 4, 1),
    ("wc", 2, 1, 1), ("p", 2, 1, 0), ("wc", 3, 2, 1), ("p", 3, 2, 0), ("wc", 2, 2, 2), ("wc", 2, 2, 0),
    ("wp", 3, 2, 1), ("wp", 1, 2, 1), ("g", 2, 2), ("wr", 3, 3), ("wr", 5, 3), ("r", 5, 3, 4, 1), ("wp", 2, 3, 0),
    ("wp", 1, 2, 0), ("wp", 2, 1, 1), ("wp", 2, 3, 1), ("wp", 2, 1, 0), ("G", 1), ("g", 1, 0), ("wr", 4, 0),
    ("wc", 2, 2, 3), ("p", 2, 2, 1), ("wc", 2, 2, 1), ("p", 2, 2, 0), ("wp", 3, 2, 0), ("g", 1, 1), ("wr", 4, 1),
    ("wr", 4, 2), ("wp", 2, 2, 1), ("g", 1, 2), ("wr", 4, 3), ("wp", 2, 2, 0), ("G", 0), ("g", 0, 0), ("g", 0, 1),
    ("g", 0, 2), ("g", 0, 3), ("F", 0), ("R", 4, 0), ("R", 4, 1), ("R", 4, 2), ("R", 4, 3), ("g", 1, 3), ("F", 1),
    ("R", 3, 2), ("R", 3, 3), ("R", 5, 0), ("R", 5, 1), ("g", 2, 3), ("F", 2), ("R", 3, 0), ("R", 3, 1), ("R", 5, 2),
    ("R", 5, 3), ("g", 3, 2), ("R", 2, 2), ("R", 2, 3), ("R", 6, 0), ("R", 6, 1), ("g", 3, 3), ("F", 3), ("R", 2, 0),
    ("R", 2, 1), ("R", 6, 2), ("R", 6, 3), ("R", 1, 2), ("R", 7, 0), ("R", 1, 3), ("R", 7, 1), ("R", 1, 0),
    ("R", 7, 2), ("R", 1, 1), ("R", 7, 3),
]


def iota(shape, dim):
    return lax.broadcasted_iota(jnp.int32, shape, dim)


def aux_block(feats, alpha_row, probe_t, probes):
    points = feats.shape[0]
    src, lane = iota((2 * probes, AUX), 0), iota((2 * probes, AUX), 1)
    scale = 1.0 / (4 * probes)
    swapped = jnp.where(src < probes, src + probes, src - probes)
    pick = jnp.where(lane == src, 1.0, 0.0) + jnp.where(lane - 64 == swapped, -scale, 0.0)
    aux = lax.dot_general(probe_t, pick.astype(BF), TN, preferred_element_type=F32)
    spread = jnp.broadcast_to(alpha_row.astype(F32), (points, points))
    diag = jnp.where(iota((points, points), 0) == iota((points, points), 1), spread, 0.0)
    lane = iota((points, AUX), 1)
    put = jnp.where(lane == 2 * probes, 1.0, 0.0) + jnp.where(lane == 64 + 2 * probes, 0.5, 0.0)
    aux = aux + jnp.dot(diag.astype(BF), put.astype(BF), preferred_element_type=F32)
    f = feats.astype(F32)
    rest = jnp.sum(f * f, axis=1, keepdims=True)
    for k in range(3):
        part = rest.astype(BF).astype(F32)
        aux = jnp.where(lane == 100 + k, part, aux)
        rest = rest - part
    return aux


def kernel(
    probes,
    amp_ref,
    lsq_ref,
    hidden_ref,
    proj_ref,
    alpha_ref,
    probe_ref,
    gh_ref,
    gp_ref,
    rows,
    row_feat,
    cols,
    left,
    bias,
    moved,
    rsum,
    sbuf,
    rplus,
    rminus,
    terms,
    pbuf,
    xrec,
    prec,
    zbuf,
    zrec,
    fbuf,
    frec,
    row_send,
    row_recv,
    col_send,
    col_recv,
    part_send,
    part_recv,
    rs_send,
    rs_recv,
    pair_send,
    pair_recv,
    p_send,
    p_recv,
    z_send,
    z_recv,
    f_send,
    f_recv,
):
    pts, hid = hidden_ref.shape
    feat = proj_ref.shape[1]
    width = feat + AUX
    half, quarter, piece = pts // 2, pts // 4, pts // PARTS
    m = 2 * pts

    r, c = lax.axis_index("row"), lax.axis_index("col")
    k, z, y_hi = r % 2, (r // 2) % NZ, r // (2 * NZ)
    x, y_lo = c // 2, c % 2
    y = y_hi * 2 + y_lo

    def dev(dx, dy, dz, flip=0):
        xx, yy, zz = (x + dx) % NX, (y + dy) % NY, (z + dz) % NZ
        kk = (1 - k) if flip else k
        return (((yy // 2) * NZ + zz) * 2 + kk, xx * 2 + yy % 2)

    plane = (dev(-1, 0, 0), dev(1, 0, 0), dev(0, -1, 0), dev(0, 1, 0))
    line = (dev(0, 0, -1), dev(0, 0, 1))
    partner = dev(0, 0, 0, 1)

    barrier = pltpu.get_barrier_semaphore()
    for peer in (*plane, *line, partner):
        pl.semaphore_signal(barrier, inc=1, device_id=peer, device_id_type=MESH)

    feats = jnp.dot(hidden_ref[...], proj_ref[...], preferred_element_type=F32).astype(BF)
    aux = aux_block(feats, alpha_ref[...], probe_ref[...], probes).astype(BF)
    own = pl.ds(SLOTS.index((0, 0, 0)) * pts, pts)
    cols[own, 0:feat] = feats
    cols[own, feat:width] = aux
    own = pl.ds(POS[0] * pts, pts)
    rows[own, 0:hid] = hidden_ref[...]
    rows[own, hid : hid + AUX] = aux

    pl.semaphore_wait(barrier, 7)

    sends = []
    used = {}

    def send(src, dst, sems, recv_sem, to):
        if isinstance(sems, tuple):
            sem = sems[0].at[sems[1:]]
        else:
            sem = sems.at[used.setdefault(id(sems), 0)]
            used[id(sems)] += 1
        copy = pltpu.make_async_remote_copy(
            src_ref=src,
            dst_ref=dst,
            send_sem=sem,
            recv_sem=recv_sem,
            device_id=to,
            device_id_type=MESH,
        )
        copy.start()
        sends.append(copy)

    def arrived(dst, recv_sem):
        pltpu.make_async_remote_copy(
            src_ref=dst,
            dst_ref=dst,
            send_sem=recv_sem,
            recv_sem=recv_sem,
            device_id=partner,
            device_id_type=MESH,
        ).wait_recv()

    def row_part(d, q):
        return rows.at[pl.ds(POS[d] * pts + q * quarter, quarter), :]

    def col_part(core, dx, dy, q, n):
        start = SLOTS.index((core, dx, dy)) * pts + q * quarter
        return cols.at[pl.ds(start, n * quarter), :]

    scale = math.log2(math.e) / lsq_ref[0]
    final = 2.0 * amp_ref[0] / lsq_ref[0]
    lane16 = iota((16, AUX), 1)
    picks = jnp.where((lane16 >= 100) & (lane16 < 103), 1.0, 0.0).astype(BF)

    def prepare(g):
        rs = pl.ds(g * m, m)
        row_feat[rs, :] = jnp.dot(
            rows[rs, 0:hid], proj_ref[...], preferred_element_type=F32
        ).astype(BF)
        lane = iota((m, AUX), 1)
        raw = rows[rs, hid : hid + AUX].astype(F32)
        norms = jnp.where((lane >= 100) & (lane < 103), raw, 0.0)
        bias[rs, :] = jnp.sum(norms, axis=1, keepdims=True) * (-0.5 * scale)
        turned = pltpu.roll(raw, 64, 1)
        factors = jnp.where((lane >= 64) & (lane <= 64 + 2 * probes), turned, 0.0)
        left[rs, :] = factors.astype(BF)

    def chunk(g, first, n, fresh):
        rs, count = pl.ds(g * m, m), n * CHUNK
        cs = pl.ds(first * CHUNK, count)
        col_f = cols[cs, 0:feat]
        col_a = cols[cs, feat:width]
        sq = lax.dot_general(picks, col_a, NT, preferred_element_type=F32)[0:1, :]
        inner = lax.dot_general(row_feat[rs, :], col_f, NT, preferred_element_type=F32)
        gmat = lax.dot_general(left[rs, :], col_a, NT, preferred_element_type=F32)
        expo = inner * scale + (bias[rs, :] + sq * (-0.5 * scale))
        weight = gmat * jnp.exp2(expo)
        total = weight[:, :128]
        for t in range(1, count // 128):
            total = total + weight[:, t * 128 : (t + 1) * 128]
        term = jnp.dot(weight.astype(BF), col_f, preferred_element_type=F32)
        if fresh:
            rsum[rs, :] = total
            moved[rs, :] = term
        else:
            rsum[rs, :] += total
            moved[rs, :] += term

    def finish(g, fresh):
        rs = pl.ds(g * m, m)
        rowsum = jnp.sum(rsum[rs, :], axis=1, keepdims=True)
        value = moved[rs, :] - rowsum * row_feat[rs, :].astype(F32)
        moved[rs, :] = value
        term = lax.dot_general(rows[rs, 0:hid], value.astype(BF), TN, preferred_element_type=F32)
        terms[...] = term if fresh else terms[...] + term

    def pass_on(d, i):
        up = d < 4 or (d == 4 and i < PARTS // 2)
        dst, way = (rplus, 0) if up else (rminus, 1)
        step = 4 - d if up else d - 4
        rs = pl.ds(POS[d] * pts + i * piece, piece)
        ps = pl.ds(i * piece, piece)
        value = moved[rs, :]
        if step > 1 or (step == 1 and up == (i < PARTS // 2)):
            arrived(dst.at[step - 1, ps, :], rs_recv.at[way, step - 1, i])
            value = value + dst[step - 1, ps, :].astype(F32)
        sbuf[rs, :] = value.astype(BF)
        send(sbuf.at[rs, :], dst.at[step, ps, :], rs_send, rs_recv.at[way, step, i], line[up])

    def row_step(op):
        if op[0] == "wr":
            arrived(row_part(*op[1:]), row_recv.at[op[1:]])
        else:
            d, q, to_d, up = op[1:]
            send(row_part(d, q), row_part(to_d, q), row_send, row_recv.at[to_d, q], line[up])

    def col_step(op):
        if op[0] == "wc":
            arrived(col_part(0, *op[1:], 1), col_recv.at[op[1:]])
        elif op[0] == "c":
            dx, dy, q, to_dx, to_dy, way = op[1:]
            dst = col_part(0, to_dx, to_dy, q, 1)
            send(col_part(0, dx, dy, q, 1), dst, col_send, col_recv.at[to_dx, to_dy, q], plane[way])
        else:
            dx, dy, h = op[1:]
            dst = col_part(1, dx, dy, 2 * h, 2)
            if op[0] == "wp":
                arrived(dst, part_recv.at[dx, dy, h])
            else:
                src = col_part(0, dx, dy, 2 * h, 2)
                send(src, dst, part_send, part_recv.at[dx, dy, h], partner)

    seen, finished = set(), 0
    at = 0
    while finished < GROUPS:
        op = PLAN[at]
        at += 1
        if op[0] == "G":
            prepare(op[1])
        elif op[0] == "g":
            g, j = op[1:]
            n = 1
            while n < 2 and PLAN[at] == ("g", g, j + n):
                at, n = at + 1, n + 1
            chunk(g, j, n, g not in seen)
            seen.add(g)
        elif op[0] == "F":
            finish(op[1], finished == 0)
            finished += 1
        elif op[0] == "R":
            pass_on(*op[1:])
        elif op[0] in ("r", "wr"):
            row_step(op)
        else:
            col_step(op)

    size = hid // (4 * NZ)
    for hi in range(2):
        for zz in range(NZ):
            for core in range(2):
                start = ((hi * NZ + zz) * 2 + core) * size
                pbuf[hi, core, zz] = (terms[start : start + size, :] * final).astype(BF)
    zs = pl.ds(k * (NZ // 2), NZ // 2)
    others = pl.ds((1 - k) * (NZ // 2), NZ // 2)
    send(pbuf.at[:, :, others], xrec, (pair_send, 0), pair_recv.at[0], partner)
    arrived(xrec, pair_recv.at[0])
    both = pbuf[:, :, zs].astype(F32) + xrec[...].astype(F32)
    pbuf[:, :, zs] = both.astype(BF)

    def portion(xx, yy):
        return yy // 2, yy % 2, zs, slice(None), pl.ds(pl.multiple_of(xx * 128, 128), 128)

    for dx in range(NX):
        for dy in range(NY):
            if dx or dy:
                to = ((NX - dx) % NX, (NY - dy) % NY)
                send(
                    pbuf.at[portion((x + dx) % NX, (y + dy) % NY)],
                    prec.at[to[0], to[1]],
                    (p_send, dx, dy),
                    p_recv.at[to[0], to[1]],
                    dev(dx, dy, 0),
                )

    for op in PLAN[at:]:
        pass_on(*op[1:])
    for i in range(PARTS):
        ps = pl.ds(i * piece, piece)
        arrived(rplus.at[3, ps, :], rs_recv.at[0, 3, i])
        arrived(rminus.at[3, ps, :], rs_recv.at[1, 3, i])
    total = moved[0:pts, :] + rplus[3].astype(F32) + rminus[3].astype(F32)
    grad = (total * final).astype(BF)
    gh_ref[...] = lax.dot_general(grad, proj_ref[...], NT, preferred_element_type=F32).astype(BF)

    share = pbuf[portion(x, y)].astype(F32)
    for dx in range(NX):
        for dy in range(NY):
            if dx or dy:
                arrived(prec.at[dx, dy], p_recv.at[dx, dy])
                share = share + prec[dx, dy].astype(F32)
    zbuf[...] = share.astype(BF)

    gathers = k == z // (NZ // 2)
    later = []

    def send_if(cond, src, dst, send_sem, recv_sem, to):
        copy = pltpu.make_async_remote_copy(
            src_ref=src,
            dst_ref=dst,
            send_sem=send_sem,
            recv_sem=recv_sem,
            device_id=to,
            device_id_type=MESH,
        )

        @pl.when(cond)
        def _():
            copy.start()

        later.append((cond, copy))

    for dz in range(1, NZ):
        zz = (z + dz) % NZ
        send_if(
            zz // (NZ // 2) == k,
            zbuf.at[zz % (NZ // 2)],
            zrec.at[NZ - dz],
            z_send.at[dz],
            z_recv.at[NZ - dz],
            dev(0, 0, dz),
        )

    @pl.when(gathers)
    def _():
        total = zbuf[z % (NZ // 2)].astype(F32)
        for dz in range(1, NZ):
            arrived(zrec.at[dz], z_recv.at[dz])
            total = total + zrec[dz].astype(F32)
        fbuf[...] = total

    mine = y_lo == k
    for dx in range(NX):
        for flip in range(2):
            xx, yy = (x + dx) % NX, y_hi * 2 + (y_lo if flip == 0 else 1 - y_lo)
            to = ((y_hi * NZ + z) * 2 + y_lo, xx * 2 + yy % 2)
            cond = gathers if dx or flip else gathers & jnp.logical_not(mine)
            slot = (NX - dx) % NX
            send_if(cond, fbuf, frec.at[slot], f_send.at[dx, flip], f_recv.at[slot], to)

    @pl.when(gathers & mine)
    def _():
        frec[0] = fbuf[...]

    for dx in range(NX):
        if dx == 0:

            @pl.when(jnp.logical_not(gathers & mine))
            def _():
                arrived(frec.at[0], f_recv.at[0])

        else:
            arrived(frec.at[dx], f_recv.at[dx])
        gp_ref[:, pl.ds(pl.multiple_of((x + dx) % NX * 128, 128), 128)] = frec[dx]

    for copy in sends:
        copy.wait_send()
    for cond, copy in later:

        @pl.when(cond)
        def _():
            copy.wait_send()


def fused(hidden, projection, alpha, probe_pairs, amplitude, length_sq):
    pts, hid = hidden.shape
    feat = projection.shape[1]
    probes = probe_pairs.shape[1] // 2
    width = feat + AUX
    n_rows, n_cols = NZ * pts, 2 * NX * NY * pts
    size = hid // (4 * NZ)
    vmem = pl.BlockSpec(memory_space=pltpu.VMEM)
    smem = pl.BlockSpec(memory_space=pltpu.SMEM)
    dma = pltpu.SemaphoreType.DMA
    return pl.pallas_call(
        functools.partial(kernel, probes),
        out_shape=(
            jax.ShapeDtypeStruct((pts, hid), BF),
            jax.ShapeDtypeStruct((hid // (4 * NZ), feat), F32),
        ),
        in_specs=[smem, smem, vmem, vmem, vmem, vmem],
        out_specs=(vmem, vmem),
        scratch_shapes=[
            pltpu.VMEM((n_rows, hid + AUX), BF),
            pltpu.VMEM((n_rows, feat), BF),
            pltpu.VMEM((n_cols, width), BF),
            pltpu.VMEM((n_rows, AUX), BF),
            pltpu.VMEM((n_rows, 1), F32),
            pltpu.VMEM((n_rows, feat), F32),
            pltpu.VMEM((n_rows, 128), F32),
            pltpu.VMEM((n_rows, feat), BF),
            pltpu.VMEM((4, pts, feat), BF),
            pltpu.VMEM((4, pts, feat), BF),
            pltpu.VMEM((hid, feat), F32),
            pltpu.VMEM((2, 2, NZ, size, feat), BF),
            pltpu.VMEM((2, 2, NZ // 2, size, feat), BF),
            pltpu.VMEM((NX, NY, NZ // 2, size, 128), BF),
            pltpu.VMEM((NZ // 2, size, 128), BF),
            pltpu.VMEM((NZ, size, 128), BF),
            pltpu.VMEM((size, 128), F32),
            pltpu.VMEM((NX, size, 128), F32),
            dma((28,)),
            dma((NZ, 4)),
            dma((60,)),
            dma((NX, NY, 4)),
            dma((32,)),
            dma((NX, NY, 2)),
            dma((7 * PARTS,)),
            dma((2, 4, PARTS)),
            dma((1,)),
            dma((1,)),
            dma((NX, NY)),
            dma((NX, NY)),
            dma((NZ,)),
            dma((NZ,)),
            dma((NX, 2)),
            dma((NX,)),
        ],
        compiler_params=pltpu.CompilerParams(
            collective_id=0, has_side_effects=True, vmem_limit_bytes=56 << 20
        ),
        name="fused",
    )(amplitude, length_sq, hidden, projection, alpha[None, :], probe_pairs.T)


def per_device(hidden, projection, alpha, probe_pairs, amplitude, length_sq):
    return fused(hidden, projection, alpha, probe_pairs, amplitude, length_sq)


def solution(mesh):
    placed = (P(("row", "col"), None), P(), P(("row", "col")), P(("row", "col"), None), P(), P())
    return jax.shard_map(
        per_device,
        mesh=mesh,
        in_specs=placed,
        out_specs=(P(("row", "col"), None), P("row", None)),
        check_vma=False,
    )
```

```python
import functools
import math

import jax
import jax.numpy as jnp
from jax import lax
from jax.experimental import pallas as pl
from jax.experimental.pallas import tpu as pltpu
from jax.sharding import PartitionSpec as P

MESH = pl.DeviceIdType.MESH
NT = (((1,), (1,)), ((), ()))
TN = (((0,), (0,)), ((), ()))
BF, F32 = jnp.bfloat16, jnp.float32

NX, NY, NZ = 4, 4, 8
AUX = 128
POS = {0: 0, 4: 1, 3: 2, 5: 3, 2: 4, 6: 5, 1: 6, 7: 7}
GROUPS = 4
CHUNK = 1024
PARTS = 4
SLOTS = [
    (0, 0, 0), (1, 0, 0), (0, 0, 1), (0, 0, 3), (0, 1, 0), (0, 3, 0), (1, 0, 1), (1, 0, 3),
    (1, 1, 0), (1, 3, 0), (0, 1, 1), (0, 1, 3), (0, 3, 1), (0, 3, 3), (1, 1, 1), (0, 0, 2),
    (0, 2, 0), (1, 1, 3), (1, 3, 1), (1, 3, 3), (1, 0, 2), (1, 2, 0), (0, 1, 2), (0, 2, 1),
    (0, 2, 3), (0, 3, 2), (1, 1, 2), (1, 2, 1), (1, 2, 3), (1, 3, 2), (0, 2, 2), (1, 2, 2),
]
PLAN = [
    ("r", 0, 0, 1, 0), ("r", 0, 0, 7, 1), ("r", 0, 1, 1, 0), ("r", 0, 1, 7, 1), ("r", 0, 2, 1, 0), ("r", 0, 2, 7, 1),
    ("r", 0, 3, 1, 0), ("r", 0, 3, 7, 1), ("c", 0, 0, 0, 1, 0, 0), ("c", 0, 0, 1, 1, 0, 0), ("c", 0, 0, 2, 0, 1, 2),
    ("c", 0, 0, 3, 0, 1, 2), ("c", 0, 0, 0, 3, 0, 1), ("c", 0, 0, 1, 3, 0, 1), ("c", 0, 0, 2, 0, 3, 3),
    ("c", 0, 0, 3, 0, 3, 3), ("c", 0, 0, 0, 0, 1, 2), ("c", 0, 0, 1, 0, 1, 2), ("c", 0, 0, 2, 1, 0, 0),
    ("c", 0, 0, 3, 1, 0, 0), ("c", 0, 0, 0, 0, 3, 3), ("c", 0, 0, 1, 0, 3, 3), ("c", 0, 0, 2, 3, 0, 1),
    ("c", 0, 0, 3, 3, 0, 1), ("p", 0, 0, 0), ("p", 0, 0, 1), ("wp", 0, 0, 0), ("wp", 0, 0, 1), ("wr", 1, 0),
    ("r", 1, 0, 2, 0), ("wr", 7, 0), ("r", 7, 0, 6, 1), ("wc", 0, 1, 2), ("c", 0, 1, 2, 0, 2, 2),
    ("c", 0, 1, 2, 1, 1, 0), ("c", 0, 1, 2, 3, 1, 1), ("wc", 0, 3, 2), ("c", 0, 3, 2, 1, 3, 0),
    ("c", 0, 3, 2, 3, 3, 1), ("wc", 1, 0, 0), ("c", 1, 0, 0, 2, 0, 0), ("c", 1, 0, 0, 1, 1, 2),
    ("c", 1, 0, 0, 1, 3, 3), ("wc", 3, 0, 0), ("c", 3, 0, 0, 3, 1, 2), ("c", 3, 0, 0, 3, 3, 3), ("wc", 0, 1, 3),
    ("c", 0, 1, 3, 1, 1, 0), ("c", 0, 1, 3, 3, 1, 1), ("p", 0, 1, 1), ("wc", 0, 3, 3), ("c", 0, 3, 3, 0, 2, 3),
    ("c", 0, 3, 3, 1, 3, 0), ("c", 0, 3, 3, 3, 3, 1), ("p", 0, 3, 1), ("wc", 1, 0, 1), ("c", 1, 0, 1, 1, 1, 2),
    ("c", 1, 0, 1, 1, 3, 3), ("p", 1, 0, 0), ("wc", 3, 0, 1), ("c", 3, 0, 1, 2, 0, 1), ("c", 3, 0, 1, 3, 1, 2),
    ("c", 3, 0, 1, 3, 3, 3), ("p", 3, 0, 0), ("wr", 1, 1), ("r", 1, 1, 2, 0), ("wr", 7, 1), ("r", 7, 1, 6, 1),
    ("wc", 0, 1, 0), ("c", 0, 1, 0, 0, 2, 2), ("wc", 0, 3, 0), ("wc", 1, 0, 2), ("c", 1, 0, 2, 2, 0, 0),
    ("wc", 3, 0, 2), ("wp", 0, 1, 1), ("wr", 1, 2), ("r", 1, 2, 2, 0), ("wr", 7, 2), ("r", 7, 2, 6, 1),
    ("wp", 0, 3, 1), ("wc", 0, 1, 1), ("p", 0, 1, 0), ("wc", 0, 3, 1), ("c", 0, 3, 1, 0, 2, 3), ("p", 0, 3, 0),
    ("wc", 1, 0, 3), ("p", 1, 0, 1), ("wc", 3, 0, 3), ("c", 3, 0, 3, 2, 0, 1), ("p", 3, 0, 1), ("wp", 1, 0, 0),
    ("wp", 3, 0, 0), ("wr", 1, 3), ("r", 1, 3, 2, 0), ("wr", 7, 3), ("r", 7, 3, 6, 1), ("wc", 0, 2, 2),
    ("c", 0, 2, 2, 1, 2, 0), ("c", 0, 2, 2, 3, 2, 1), ("wc", 1, 1, 2), ("c", 1, 1, 2, 2, 1, 0), ("wc", 1, 3, 0),
    ("wc", 3, 1, 2), ("wp", 0, 1, 0), ("wp", 0, 3, 0), ("G", 3), ("g", 3, 0), ("wr", 2, 0), ("r", 2, 0, 3, 0),
    ("wr", 6, 0), ("r", 6, 0, 5, 1), ("wc", 0, 2, 3), ("c", 0, 2, 3, 1, 2, 0), ("c", 0, 2, 3, 3, 2, 1),
    ("p", 0, 2, 1), ("wc", 2, 0, 0), ("c", 2, 0, 0, 2, 1, 2), ("c", 2, 0, 0, 2, 3, 3), ("wc", 1, 1, 0),
    ("c", 1, 1, 0, 1, 2, 2), ("wc", 1, 3, 2), ("c", 1, 3, 2, 2, 3, 0), ("wc", 3, 3, 0), ("wc", 3, 3, 2),
    ("wc", 3, 1, 0), ("c", 3, 1, 0, 3, 2, 2), ("wc", 3, 1, 3), ("c", 3, 1, 3, 2, 1, 1), ("p", 3, 1, 1),
    ("wp", 1, 0, 1), ("wp", 3, 0, 1), ("wr", 2, 1), ("r", 2, 1, 3, 0), ("wr", 6, 1), ("r", 6, 1, 5, 1),
    ("wc", 1, 1, 1), ("p", 1, 1, 0), ("wc", 1, 1, 3), ("p", 1, 1, 1), ("wc", 1, 3, 1), ("c", 1, 3, 1, 1, 2, 3),
    ("p", 1, 3, 0), ("wc", 3, 3, 3), ("c", 3, 3, 3, 2, 3, 1), ("p", 3, 3, 1), ("wp", 0, 2, 1), ("wc", 2, 0, 1),
    ("c", 2, 0, 1, 2, 1, 2), ("c", 2, 0, 1, 2, 3, 3), ("p", 2, 0, 0), ("wc", 1, 3, 3), ("p", 1, 3, 1),
    ("wc", 3, 1, 1), ("p", 3, 1, 0), ("wc", 3, 3, 1), ("c", 3, 3, 1, 3, 2, 3), ("p", 3, 3, 0), ("wp", 3, 1, 1),
    ("wr", 2, 2), ("r", 2, 2, 3, 0), ("wr", 6, 2), ("r", 6, 2, 5, 1), ("wp", 1, 1, 0), ("wp", 1, 1, 1),
    ("wc", 0, 2, 0), ("wc", 0, 2, 1), ("p", 0, 2, 0), ("wc", 2, 0, 2), ("wc", 2, 0, 3), ("p", 2, 0, 1), ("g", 3, 1),
    ("wr", 2, 3), ("r", 2, 3, 3, 0), ("wr", 6, 3), ("r", 6, 3, 5, 1), ("wc", 1, 2, 2), ("c", 1, 2, 2, 2, 2, 0),
    ("wc", 3, 2, 2), ("wp", 1, 3, 0), ("wc", 2, 1, 0), ("c", 2, 1, 0, 2, 2, 2), ("wc", 2, 3, 0), ("wp", 3, 3, 1),
    ("wp", 2, 0, 0), ("wp", 1, 3, 1), ("G", 2), ("g", 2, 0), ("wr", 3, 0), ("r", 3, 0, 4, 0), ("wr", 5, 0),
    ("wc", 3, 2, 3), ("c", 3, 2, 3, 2, 2, 1), ("p", 3, 2, 1), ("wc", 2, 1, 2), ("wc", 1, 2, 0), ("wc", 1, 2, 1),
    ("p", 1, 2, 0), ("wp", 3, 1, 0), ("wp", 3, 3, 0), ("wp", 0, 2, 0), ("wp", 2, 0, 1), ("g", 2, 1), ("wr", 3, 1),
    ("r", 3, 1, 4, 0), ("wr", 5, 1), ("wc", 1, 2, 3), ("p", 1, 2, 1), ("wc", 2, 3, 1), ("c", 2, 3, 1, 2, 2, 3),
    ("p", 2, 3, 0), ("wc", 2, 1, 3), ("p", 2, 1, 1), ("wc", 3, 2, 0), ("wc", 2, 3, 2), ("wc", 2, 3, 3),
    ("p", 2, 3, 1), ("wc", 2, 1, 1), ("p", 2, 1, 0), ("wc", 3, 2, 1), ("p", 3, 2, 0), ("g", 2, 2), ("wr", 3, 2),
    ("wr", 5, 2), ("r", 5, 2, 4, 1), ("wc", 2, 2, 2), ("wc", 2, 2, 0), ("wp", 3, 2, 1), ("wp", 1, 2, 0), ("g", 3, 2),
    ("wr", 3, 3), ("wr", 5, 3), ("r", 5, 3, 4, 1), ("wp", 1, 2, 1), ("wp", 2, 3, 0), ("wp", 2, 1, 1), ("wp", 2, 3, 1),
    ("G", 1), ("g", 1, 0), ("wr", 4, 0), ("wc", 2, 2, 3), ("p", 2, 2, 1), ("wc", 2, 2, 1), ("p", 2, 2, 0),
    ("wp", 2, 1, 0), ("wp", 3, 2, 0), ("g", 1, 1), ("wr", 4, 1), ("g", 1, 2), ("wr", 4, 2), ("wp", 2, 2, 1),
    ("wp", 2, 2, 0), ("g", 1, 3), ("F", 1), ("wr", 4, 3), ("R", 3, 2), ("R", 3, 3), ("R", 5, 0), ("R", 5, 1),
    ("G", 0), ("g", 0, 0), ("g", 0, 1), ("g", 0, 2), ("g", 0, 3), ("F", 0), ("R", 4, 0), ("R", 4, 1), ("R", 4, 2),
    ("R", 4, 3), ("g", 2, 3), ("F", 2), ("R", 2, 2), ("R", 2, 3), ("R", 6, 0), ("R", 6, 1), ("g", 3, 3), ("F", 3),
    ("R", 3, 0), ("R", 5, 2), ("R", 3, 1), ("R", 5, 3), ("R", 1, 2), ("R", 7, 0), ("R", 1, 3), ("R", 7, 1),
    ("R", 2, 0), ("R", 6, 2), ("R", 2, 1), ("R", 6, 3), ("R", 1, 0), ("R", 7, 2), ("R", 1, 1), ("R", 7, 3),
]


def iota(shape, dim):
    return lax.broadcasted_iota(jnp.int32, shape, dim)


def factor_block(alpha_row, probe_t, probes):
    points = alpha_row.shape[1]
    src, lane = iota((2 * probes, AUX), 0), iota((2 * probes, AUX), 1)
    scale = 1.0 / (4 * probes)
    swapped = jnp.where(src < probes, src + probes, src - probes)
    pick = jnp.where(lane == src, 1.0, 0.0) + jnp.where(lane - 64 == swapped, -scale, 0.0)
    aux = lax.dot_general(probe_t, pick.astype(BF), TN, preferred_element_type=F32)
    spread = jnp.broadcast_to(alpha_row.astype(F32), (points, points))
    diag = jnp.where(iota((points, points), 0) == iota((points, points), 1), spread, 0.0)
    lane = iota((points, AUX), 1)
    put = jnp.where(lane == 2 * probes, 1.0, 0.0) + jnp.where(lane == 64 + 2 * probes, 0.5, 0.0)
    aux = aux + jnp.dot(diag.astype(BF), put.astype(BF), preferred_element_type=F32)
    return aux


def norms_of(feats):
    f = feats.astype(F32)
    return jnp.sum(f * f, axis=1, keepdims=True)


def with_norms(factors, norms):
    lane = iota(factors.shape, 1)
    for k in range(3):
        part = norms.astype(BF).astype(F32)
        factors = jnp.where(lane == 100 + k, part, factors)
        norms = norms - part
    return factors


def kernel(
    probes,
    amp_ref,
    lsq_ref,
    hidden_hbm,
    proj_hbm,
    alpha_hbm,
    probe_hbm,
    gh_ref,
    gp_ref,
    rows,
    row_feat,
    cols,
    left,
    bias,
    moved,
    rsum,
    sbuf,
    rplus,
    rminus,
    terms,
    pbuf,
    xrec,
    prec,
    zbuf,
    zrec,
    fbuf,
    frec,
    row_send,
    row_recv,
    col_send,
    col_recv,
    part_send,
    part_recv,
    rs_send,
    rs_recv,
    pair_send,
    pair_recv,
    p_send,
    p_recv,
    z_send,
    z_recv,
    f_send,
    f_recv,
    proj_ref,
    alpha_ref,
    probe_ref,
    in_sem,
):
    pts, hid = hidden_hbm.shape
    feat = proj_ref.shape[1]
    width = feat + AUX
    half, quarter, piece = pts // 2, pts // 4, pts // PARTS
    m = 2 * pts

    r, c = lax.axis_index("row"), lax.axis_index("col")
    k, z, y_hi = r % 2, (r // 2) % NZ, r // (2 * NZ)
    x, y_lo = c // 2, c % 2
    y = y_hi * 2 + y_lo

    def dev(dx, dy, dz, flip=0):
        xx, yy, zz = (x + dx) % NX, (y + dy) % NY, (z + dz) % NZ
        kk = (1 - k) if flip else k
        return (((yy // 2) * NZ + zz) * 2 + kk, xx * 2 + yy % 2)

    plane = (dev(-1, 0, 0), dev(1, 0, 0), dev(0, -1, 0), dev(0, 1, 0))
    line = (dev(0, 0, -1), dev(0, 0, 1))
    partner = dev(0, 0, 0, 1)

    own_rows = pl.ds(POS[0] * pts, pts)
    hidden_ref = rows.at[own_rows, pl.ds(0, hid)]
    loads = [
        pltpu.make_async_copy(src, dst, in_sem.at[i])
        for i, (src, dst) in enumerate(
            (
                (hidden_hbm, hidden_ref),
                (alpha_hbm, alpha_ref),
                (probe_hbm, probe_ref),
                (proj_hbm, proj_ref),
            )
        )
    ]
    for load in loads:
        load.start()

    barrier = pltpu.get_barrier_semaphore()
    for peer in (*plane, *line, partner):
        pl.semaphore_signal(barrier, inc=1, device_id=peer, device_id_type=MESH)

    for load in loads[1:3]:
        load.wait()
    factors = factor_block(alpha_ref[...], probe_ref[...], probes)
    rows[own_rows, hid : hid + AUX] = factors.astype(BF)
    loads[0].wait()

    pl.semaphore_wait(barrier, 7)

    sends = []
    used = {}

    def send(src, dst, sems, recv_sem, to):
        if isinstance(sems, tuple):
            sem = sems[0].at[sems[1:]]
        else:
            sem = sems.at[used.setdefault(id(sems), 0)]
            used[id(sems)] += 1
        copy = pltpu.make_async_remote_copy(
            src_ref=src,
            dst_ref=dst,
            send_sem=sem,
            recv_sem=recv_sem,
            device_id=to,
            device_id_type=MESH,
        )
        copy.start()
        sends.append(copy)

    def arrived(dst, recv_sem):
        pltpu.make_async_remote_copy(
            src_ref=dst,
            dst_ref=dst,
            send_sem=recv_sem,
            recv_sem=recv_sem,
            device_id=partner,
            device_id_type=MESH,
        ).wait_recv()

    def row_part(d, q):
        return rows.at[pl.ds(POS[d] * pts + q * quarter, quarter), :]

    def col_part(core, dx, dy, q, n):
        start = SLOTS.index((core, dx, dy)) * pts + q * quarter
        return cols.at[pl.ds(start, n * quarter), :]

    scale = math.log2(math.e) / lsq_ref[0]
    final = 2.0 * amp_ref[0] / lsq_ref[0]
    lane16 = iota((16, AUX), 1)
    picks = jnp.where((lane16 >= 100) & (lane16 < 103), 1.0, 0.0).astype(BF)

    def prepare(g):
        rs = pl.ds(g * m, m)
        feats = jnp.dot(rows[rs, 0:hid], proj_ref[...], preferred_element_type=F32).astype(BF)
        row_feat[rs, :] = feats
        bias[rs, :] = norms_of(feats) * (-0.5 * scale)
        lane = iota((m, AUX), 1)
        raw = rows[rs, hid : hid + AUX].astype(F32)
        turned = pltpu.roll(raw, 64, 1)
        factors = jnp.where((lane >= 64) & (lane <= 64 + 2 * probes), turned, 0.0)
        left[rs, :] = factors.astype(BF)

    def chunk(g, first, n, fresh):
        rs, count = pl.ds(g * m, m), n * CHUNK
        cs = pl.ds(first * CHUNK, count)
        col_f = cols[cs, 0:feat]
        col_a = cols[cs, feat:width]
        sq = lax.dot_general(picks, col_a, NT, preferred_element_type=F32)[0:1, :]
        inner = lax.dot_general(row_feat[rs, :], col_f, NT, preferred_element_type=F32)
        gmat = lax.dot_general(left[rs, :], col_a, NT, preferred_element_type=F32)
        expo = inner * scale + (bias[rs, :] + sq * (-0.5 * scale))
        weight = gmat * jnp.exp2(expo)
        total = weight[:, :128]
        for t in range(1, count // 128):
            total = total + weight[:, t * 128 : (t + 1) * 128]
        term = jnp.dot(weight.astype(BF), col_f, preferred_element_type=F32)
        if fresh:
            rsum[rs, :] = total
            moved[rs, :] = term
        else:
            rsum[rs, :] += total
            moved[rs, :] += term

    def finish(g, fresh):
        rs = pl.ds(g * m, m)
        rowsum = jnp.sum(rsum[rs, :], axis=1, keepdims=True)
        value = moved[rs, :] - rowsum * row_feat[rs, :].astype(F32)
        moved[rs, :] = value
        term = lax.dot_general(rows[rs, 0:hid], value.astype(BF), TN, preferred_element_type=F32)
        terms[...] = term if fresh else terms[...] + term

    def pass_on(d, i):
        up = d < 4 or (d == 4 and i < PARTS // 2)
        dst, way = (rplus, 0) if up else (rminus, 1)
        step = 4 - d if up else d - 4
        rs = pl.ds(POS[d] * pts + i * piece, piece)
        ps = pl.ds(i * piece, piece)
        value = moved[rs, :]
        if step > 1 or (step == 1 and up == (i < PARTS // 2)):
            arrived(dst.at[step - 1, ps, :], rs_recv.at[way, step - 1, i])
            value = value + dst[step - 1, ps, :].astype(F32)
        sbuf[rs, :] = value.astype(BF)
        send(sbuf.at[rs, :], dst.at[step, ps, :], rs_send, rs_recv.at[way, step, i], line[up])

    def row_step(op):
        if op[0] == "wr":
            arrived(row_part(*op[1:]), row_recv.at[op[1:]])
        else:
            d, q, to_d, up = op[1:]
            send(row_part(d, q), row_part(to_d, q), row_send, row_recv.at[to_d, q], line[up])

    def col_step(op):
        if op[0] == "wc":
            arrived(col_part(0, *op[1:], 1), col_recv.at[op[1:]])
        elif op[0] == "c":
            dx, dy, q, to_dx, to_dy, way = op[1:]
            dst = col_part(0, to_dx, to_dy, q, 1)
            send(col_part(0, dx, dy, q, 1), dst, col_send, col_recv.at[to_dx, to_dy, q], plane[way])
        else:
            dx, dy, h = op[1:]
            dst = col_part(1, dx, dy, 2 * h, 2)
            if op[0] == "wp":
                arrived(dst, part_recv.at[dx, dy, h])
            else:
                src = col_part(0, dx, dy, 2 * h, 2)
                send(src, dst, part_send, part_recv.at[dx, dy, h], partner)

    at = 0
    while PLAN[at][0] == "r":
        row_step(PLAN[at])
        at += 1
    loads[3].wait()
    feats = jnp.dot(hidden_ref[...], proj_ref[...], preferred_element_type=F32).astype(BF)
    own = pl.ds(SLOTS.index((0, 0, 0)) * pts, pts)
    cols[own, 0:feat] = feats
    cols[own, feat:width] = with_norms(factors, norms_of(feats)).astype(BF)

    seen, finished = set(), 0
    while finished < GROUPS:
        op = PLAN[at]
        at += 1
        if op[0] == "G":
            prepare(op[1])
        elif op[0] == "g":
            g, j = op[1:]
            n = 1
            while n < 2 and PLAN[at] == ("g", g, j + n):
                at, n = at + 1, n + 1
            chunk(g, j, n, g not in seen)
            seen.add(g)
        elif op[0] == "F":
            finish(op[1], finished == 0)
            finished += 1
        elif op[0] == "R":
            pass_on(*op[1:])
        elif op[0] in ("r", "wr"):
            row_step(op)
        else:
            col_step(op)

    pbuf[...] = (terms[...] * final).astype(BF).reshape(pbuf.shape)
    send(pbuf.at[:, :, 1 - k], xrec, (pair_send, 0), pair_recv.at[0], partner)
    arrived(xrec, pair_recv.at[0])
    pbuf[:, :, k] = (pbuf[:, :, k].astype(F32) + xrec[...].astype(F32)).astype(BF)

    def portion(xx, yy):
        lanes = pl.ds(pl.multiple_of(xx * 128, 128), 128)
        return yy // 2, yy % 2, k, slice(None), slice(None), lanes

    for dx in range(NX):
        for dy in range(NY):
            if dx or dy:
                to = ((NX - dx) % NX, (NY - dy) % NY)
                send(
                    pbuf.at[portion((x + dx) % NX, (y + dy) % NY)],
                    prec.at[to[0], to[1]],
                    (p_send, dx, dy),
                    p_recv.at[to[0], to[1]],
                    dev(dx, dy, 0),
                )

    for op in PLAN[at:]:
        pass_on(*op[1:])
    for i in range(PARTS):
        ps = pl.ds(i * piece, piece)
        arrived(rplus.at[3, ps, :], rs_recv.at[0, 3, i])
        arrived(rminus.at[3, ps, :], rs_recv.at[1, 3, i])
    total = moved[0:pts, :] + rplus[3].astype(F32) + rminus[3].astype(F32)
    grad = (total * final).astype(BF)
    gh_ref[...] = lax.dot_general(grad, proj_ref[...], NT, preferred_element_type=F32).astype(BF)

    share = pbuf[portion(x, y)].astype(F32)
    for dx in range(NX):
        for dy in range(NY):
            if dx or dy:
                arrived(prec.at[dx, dy], p_recv.at[dx, dy])
                share = share + prec[dx, dy].astype(F32)
    zbuf[...] = share.astype(BF)

    def falls_here(zz):
        return (zz // 4 == y_lo) & (zz % 4 // 2 == k)

    gathers = falls_here(z)
    later = []

    def send_if(cond, src, dst, send_sem, recv_sem, to):
        copy = pltpu.make_async_remote_copy(
            src_ref=src,
            dst_ref=dst,
            send_sem=send_sem,
            recv_sem=recv_sem,
            device_id=to,
            device_id_type=MESH,
        )

        @pl.when(cond)
        def _():
            copy.start()

        later.append((cond, copy))

    for dz in (4, 3, 5, 2, 6, 1, 7):
        zz = (z + dz) % NZ
        send_if(
            falls_here(zz),
            zbuf.at[zz % 2],
            zrec.at[NZ - dz],
            z_send.at[dz],
            z_recv.at[NZ - dz],
            dev(0, 0, dz),
        )

    @pl.when(gathers)
    def _():
        total = zbuf[z % 2].astype(F32)
        for dz in range(1, NZ):
            arrived(zrec.at[dz], z_recv.at[dz])
            total = total + zrec[dz].astype(F32)
        fbuf[...] = total.reshape(fbuf.shape).astype(BF)

    for flip in (1, 0):
        for dx in (2, 1, 3, 0):
            for core in range(2):
                xx, yy = (x + dx) % NX, (y_lo if flip == 0 else 1 - y_lo)
                to = ((y_hi * NZ + z) * 2 + core, xx * 2 + yy)
                slot = (NX - dx) % NX
                send_if(
                    gathers if dx or flip else gathers & (k != core),
                    fbuf.at[core],
                    frec.at[slot],
                    f_send.at[dx, flip, core],
                    f_recv.at[slot],
                    to,
                )

    @pl.when(gathers)
    def _():
        frec[0] = fbuf[k]

    for dx in range(NX):
        if dx == 0:

            @pl.when(jnp.logical_not(gathers))
            def _():
                arrived(frec.at[0], f_recv.at[0])

        else:
            arrived(frec.at[dx], f_recv.at[dx])
        gp_ref[:, pl.ds(pl.multiple_of((x + dx) % NX * 128, 128), 128)] = frec[dx].astype(F32)

    for copy in sends:
        copy.wait_send()
    for cond, copy in later:

        @pl.when(cond)
        def _():
            copy.wait_send()


def fused(hidden, projection, alpha, probe_pairs, amplitude, length_sq):
    pts, hid = hidden.shape
    feat = projection.shape[1]
    probes = probe_pairs.shape[1] // 2
    width = feat + AUX
    n_rows, n_cols = NZ * pts, 2 * NX * NY * pts
    size = hid // (4 * NZ)
    vmem = pl.BlockSpec(memory_space=pltpu.VMEM)
    hbm = pl.BlockSpec(memory_space=pltpu.HBM)
    smem = pl.BlockSpec(memory_space=pltpu.SMEM)
    dma = pltpu.SemaphoreType.DMA
    return pl.pallas_call(
        functools.partial(kernel, probes),
        out_shape=(
            jax.ShapeDtypeStruct((pts, hid), BF),
            jax.ShapeDtypeStruct((hid // (4 * NZ), feat), F32),
        ),
        in_specs=[smem, smem, hbm, hbm, hbm, hbm],
        out_specs=(vmem, vmem),
        scratch_shapes=[
            pltpu.VMEM((n_rows, hid + AUX), BF),
            pltpu.VMEM((n_rows, feat), BF),
            pltpu.VMEM((n_cols, width), BF),
            pltpu.VMEM((n_rows, AUX), BF),
            pltpu.VMEM((n_rows, 1), F32),
            pltpu.VMEM((n_rows, feat), F32),
            pltpu.VMEM((n_rows, 128), F32),
            pltpu.VMEM((n_rows, feat), BF),
            pltpu.VMEM((4, pts, feat), BF),
            pltpu.VMEM((4, pts, feat), BF),
            pltpu.VMEM((hid, feat), F32),
            pltpu.VMEM((2, 2, 2, 2, 2 * size, feat), BF),
            pltpu.VMEM((2, 2, 2, 2 * size, feat), BF),
            pltpu.VMEM((NX, NY, 2, 2 * size, 128), BF),
            pltpu.VMEM((2, 2 * size, 128), BF),
            pltpu.VMEM((NZ, 2 * size, 128), BF),
            pltpu.VMEM((2, size, 128), BF),
            pltpu.VMEM((NX, size, 128), BF),
            dma((28,)),
            dma((NZ, 4)),
            dma((60,)),
            dma((NX, NY, 4)),
            dma((32,)),
            dma((NX, NY, 2)),
            dma((7 * PARTS,)),
            dma((2, 4, PARTS)),
            dma((1,)),
            dma((1,)),
            dma((NX, NY)),
            dma((NX, NY)),
            dma((NZ,)),
            dma((NZ,)),
            dma((NX, 2, 2)),
            dma((NX,)),
            pltpu.VMEM((hid, feat), BF),
            pltpu.VMEM((1, pts), BF),
            pltpu.VMEM((2 * probes, pts), BF),
            dma((4,)),
        ],
        compiler_params=pltpu.CompilerParams(
            collective_id=0, has_side_effects=True, vmem_limit_bytes=28 << 20
        ),
        name="fused",
    )(amplitude, length_sq, *(pltpu.with_memory_space_constraint(a, pltpu.HBM) for a in (hidden, projection, alpha[None, :], probe_pairs.T)))


def per_device(hidden, projection, alpha, probe_pairs, amplitude, length_sq):
    return fused(hidden, projection, alpha, probe_pairs, amplitude, length_sq)


def solution(mesh):
    placed = (P(("row", "col"), None), P(), P(("row", "col")), P(("row", "col"), None), P(), P())
    return jax.shard_map(
        per_device,
        mesh=mesh,
        in_specs=placed,
        out_specs=(P(("row", "col"), None), P("row", None)),
        check_vma=False,
    )
```

```python
import functools
import math

import jax
import jax.numpy as jnp
from jax import lax
from jax.experimental import pallas as pl
from jax.experimental.pallas import tpu as pltpu
from jax.sharding import PartitionSpec as P

MESH = pl.DeviceIdType.MESH
NT = (((1,), (1,)), ((), ()))
TN = (((0,), (0,)), ((), ()))
BF, F32 = jnp.bfloat16, jnp.float32

NX, NY, NZ = 4, 4, 8
AUX = 128
POS = {0: 0, 4: 1, 3: 2, 5: 3, 2: 4, 6: 5, 1: 6, 7: 7}
GROUPS = 4
CHUNK = 1024
MERGE = 2
LATE = 0
PARTS = 4
ROW_PARTS = 4
SLOTS = [
    (0, 0, 0), (1, 0, 0), (0, 0, 1), (0, 0, 3), (0, 1, 0), (0, 3, 0), (1, 0, 1), (1, 0, 3),
    (1, 1, 0), (1, 3, 0), (0, 1, 1), (0, 1, 3), (0, 3, 1), (0, 3, 3), (1, 1, 1), (0, 0, 2),
    (0, 2, 0), (1, 1, 3), (1, 3, 1), (1, 3, 3), (1, 0, 2), (1, 2, 0), (0, 1, 2), (0, 2, 1),
    (0, 2, 3), (0, 3, 2), (1, 1, 2), (1, 2, 1), (1, 2, 3), (1, 3, 2), (0, 2, 2), (1, 2, 2),
]
PLAN = [
    ("r", 0, 0, 1, 0), ("r", 0, 0, 7, 1), ("r", 0, 1, 1, 0), ("r", 0, 1, 7, 1), ("r", 0, 2, 1, 0), ("r", 0, 2, 7, 1),
    ("r", 0, 3, 1, 0), ("r", 0, 3, 7, 1), ("c", 0, 0, 0, 1, 0, 0), ("c", 0, 0, 1, 1, 0, 0), ("c", 0, 0, 2, 0, 1, 2),
    ("c", 0, 0, 3, 0, 1, 2), ("c", 0, 0, 0, 3, 0, 1), ("c", 0, 0, 1, 3, 0, 1), ("c", 0, 0, 2, 0, 3, 3),
    ("c", 0, 0, 3, 0, 3, 3), ("c", 0, 0, 0, 0, 1, 2), ("c", 0, 0, 1, 0, 1, 2), ("c", 0, 0, 2, 1, 0, 0),
    ("c", 0, 0, 3, 1, 0, 0), ("c", 0, 0, 0, 0, 3, 3), ("c", 0, 0, 1, 0, 3, 3), ("c", 0, 0, 2, 3, 0, 1),
    ("c", 0, 0, 3, 3, 0, 1), ("p", 0, 0, 0), ("p", 0, 0, 1), ("wp", 0, 0, 0), ("wp", 0, 0, 1), ("wr", 1, 0),
    ("r", 1, 0, 2, 0), ("wr", 7, 0), ("r", 7, 0, 6, 1), ("wc", 0, 1, 2), ("c", 0, 1, 2, 0, 2, 2),
    ("c", 0, 1, 2, 1, 1, 0), ("c", 0, 1, 2, 3, 1, 1), ("wc", 0, 3, 2), ("c", 0, 3, 2, 1, 3, 0),
    ("c", 0, 3, 2, 3, 3, 1), ("wc", 1, 0, 0), ("c", 1, 0, 0, 2, 0, 0), ("c", 1, 0, 0, 1, 1, 2),
    ("c", 1, 0, 0, 1, 3, 3), ("wc", 3, 0, 0), ("c", 3, 0, 0, 3, 1, 2), ("c", 3, 0, 0, 3, 3, 3), ("wc", 0, 1, 3),
    ("c", 0, 1, 3, 1, 1, 0), ("c", 0, 1, 3, 3, 1, 1), ("p", 0, 1, 1), ("wc", 0, 3, 3), ("c", 0, 3, 3, 0, 2, 3),
    ("c", 0, 3, 3, 1, 3, 0), ("c", 0, 3, 3, 3, 3, 1), ("p", 0, 3, 1), ("wc", 1, 0, 1), ("c", 1, 0, 1, 1, 1, 2),
    ("c", 1, 0, 1, 1, 3, 3), ("p", 1, 0, 0), ("wc", 3, 0, 1), ("c", 3, 0, 1, 2, 0, 1), ("c", 3, 0, 1, 3, 1, 2),
    ("c", 3, 0, 1, 3, 3, 3), ("p", 3, 0, 0), ("wr", 1, 1), ("r", 1, 1, 2, 0), ("wr", 7, 1), ("r", 7, 1, 6, 1),
    ("wc", 0, 1, 0), ("c", 0, 1, 0, 0, 2, 2), ("wc", 0, 3, 0), ("wc", 1, 0, 2), ("c", 1, 0, 2, 2, 0, 0),
    ("wc", 3, 0, 2), ("wp", 0, 1, 1), ("wr", 1, 2), ("r", 1, 2, 2, 0), ("wr", 7, 2), ("r", 7, 2, 6, 1),
    ("wp", 0, 3, 1), ("wc", 0, 1, 1), ("p", 0, 1, 0), ("wc", 0, 3, 1), ("c", 0, 3, 1, 0, 2, 3), ("p", 0, 3, 0),
    ("wc", 1, 0, 3), ("p", 1, 0, 1), ("wc", 3, 0, 3), ("c", 3, 0, 3, 2, 0, 1), ("p", 3, 0, 1), ("wp", 1, 0, 0),
    ("wp", 3, 0, 0), ("wr", 1, 3), ("r", 1, 3, 2, 0), ("wr", 7, 3), ("r", 7, 3, 6, 1), ("wc", 0, 2, 2),
    ("c", 0, 2, 2, 1, 2, 0), ("c", 0, 2, 2, 3, 2, 1), ("wc", 1, 1, 2), ("c", 1, 1, 2, 2, 1, 0), ("wc", 1, 3, 0),
    ("wc", 3, 1, 2), ("wp", 0, 1, 0), ("wp", 0, 3, 0), ("G", 3), ("g", 3, 0), ("wr", 2, 0), ("r", 2, 0, 3, 0),
    ("wr", 6, 0), ("r", 6, 0, 5, 1), ("wc", 0, 2, 3), ("c", 0, 2, 3, 1, 2, 0), ("c", 0, 2, 3, 3, 2, 1),
    ("p", 0, 2, 1), ("wc", 2, 0, 0), ("c", 2, 0, 0, 2, 1, 2), ("c", 2, 0, 0, 2, 3, 3), ("wc", 1, 1, 0),
    ("c", 1, 1, 0, 1, 2, 2), ("wc", 1, 3, 2), ("c", 1, 3, 2, 2, 3, 0), ("wc", 3, 3, 0), ("wc", 3, 3, 2),
    ("wc", 3, 1, 0), ("c", 3, 1, 0, 3, 2, 2), ("wc", 3, 1, 3), ("c", 3, 1, 3, 2, 1, 1), ("p", 3, 1, 1),
    ("wp", 1, 0, 1), ("wp", 3, 0, 1), ("wr", 2, 1), ("r", 2, 1, 3, 0), ("wr", 6, 1), ("r", 6, 1, 5, 1),
    ("wc", 1, 1, 1), ("p", 1, 1, 0), ("wc", 1, 1, 3), ("p", 1, 1, 1), ("wc", 1, 3, 1), ("c", 1, 3, 1, 1, 2, 3),
    ("p", 1, 3, 0), ("wc", 3, 3, 3), ("c", 3, 3, 3, 2, 3, 1), ("p", 3, 3, 1), ("wp", 0, 2, 1), ("wc", 2, 0, 1),
    ("c", 2, 0, 1, 2, 1, 2), ("c", 2, 0, 1, 2, 3, 3), ("p", 2, 0, 0), ("wc", 1, 3, 3), ("p", 1, 3, 1),
    ("wc", 3, 1, 1), ("p", 3, 1, 0), ("wc", 3, 3, 1), ("c", 3, 3, 1, 3, 2, 3), ("p", 3, 3, 0), ("wp", 3, 1, 1),
    ("wr", 2, 2), ("r", 2, 2, 3, 0), ("wr", 6, 2), ("r", 6, 2, 5, 1), ("wp", 1, 1, 0), ("wp", 1, 1, 1),
    ("wc", 0, 2, 0), ("wc", 0, 2, 1), ("p", 0, 2, 0), ("wc", 2, 0, 2), ("wc", 2, 0, 3), ("p", 2, 0, 1), ("g", 3, 1),
    ("wr", 2, 3), ("r", 2, 3, 3, 0), ("wr", 6, 3), ("r", 6, 3, 5, 1), ("wc", 1, 2, 2), ("c", 1, 2, 2, 2, 2, 0),
    ("wc", 3, 2, 2), ("wp", 1, 3, 0), ("wc", 2, 1, 0), ("c", 2, 1, 0, 2, 2, 2), ("wc", 2, 3, 0), ("wp", 3, 3, 1),
    ("wp", 2, 0, 0), ("wp", 1, 3, 1), ("G", 2), ("g", 2, 0), ("wr", 3, 0), ("r", 3, 0, 4, 0), ("wr", 5, 0),
    ("wc", 3, 2, 3), ("c", 3, 2, 3, 2, 2, 1), ("p", 3, 2, 1), ("wc", 2, 1, 2), ("wc", 1, 2, 0), ("wc", 1, 2, 1),
    ("p", 1, 2, 0), ("wp", 3, 1, 0), ("wp", 3, 3, 0), ("wp", 0, 2, 0), ("wp", 2, 0, 1), ("g", 2, 1), ("wr", 3, 1),
    ("r", 3, 1, 4, 0), ("wr", 5, 1), ("wc", 1, 2, 3), ("p", 1, 2, 1), ("wc", 2, 3, 1), ("c", 2, 3, 1, 2, 2, 3),
    ("p", 2, 3, 0), ("wc", 2, 1, 3), ("p", 2, 1, 1), ("wc", 3, 2, 0), ("wc", 2, 3, 2), ("wc", 2, 3, 3),
    ("p", 2, 3, 1), ("wc", 2, 1, 1), ("p", 2, 1, 0), ("wc", 3, 2, 1), ("p", 3, 2, 0), ("g", 2, 2), ("wr", 3, 2),
    ("wr", 5, 2), ("r", 5, 2, 4, 1), ("wc", 2, 2, 2), ("wc", 2, 2, 0), ("wp", 3, 2, 1), ("wp", 1, 2, 0), ("g", 3, 2),
    ("wr", 3, 3), ("wr", 5, 3), ("r", 5, 3, 4, 1), ("wp", 1, 2, 1), ("wp", 2, 3, 0), ("wp", 2, 1, 1), ("wp", 2, 3, 1),
    ("G", 1), ("g", 1, 0), ("wr", 4, 0), ("wc", 2, 2, 3), ("p", 2, 2, 1), ("wc", 2, 2, 1), ("p", 2, 2, 0),
    ("wp", 2, 1, 0), ("wp", 3, 2, 0), ("g", 1, 1), ("wr", 4, 1), ("g", 1, 2), ("wr", 4, 2), ("wp", 2, 2, 1),
    ("wp", 2, 2, 0), ("g", 1, 3), ("F", 1), ("wr", 4, 3), ("R", 3, 2), ("R", 3, 3), ("R", 5, 0), ("R", 5, 1),
    ("G", 0), ("g", 0, 0), ("g", 0, 1), ("g", 0, 2), ("g", 0, 3), ("F", 0), ("R", 4, 0), ("R", 4, 1), ("R", 4, 2),
    ("R", 4, 3), ("g", 2, 3), ("F", 2), ("R", 2, 2), ("R", 2, 3), ("R", 6, 0), ("R", 6, 1), ("g", 3, 3), ("F", 3),
    ("R", 3, 0), ("R", 5, 2), ("R", 3, 1), ("R", 5, 3), ("R", 1, 2), ("R", 7, 0), ("R", 1, 3), ("R", 7, 1),
    ("R", 2, 0), ("R", 6, 2), ("R", 2, 1), ("R", 6, 3), ("R", 1, 0), ("R", 7, 2), ("R", 1, 1), ("R", 7, 3),
]


def iota(shape, dim):
    return lax.broadcasted_iota(jnp.int32, shape, dim)


def factor_block(alpha_row, probe_t, probes):
    points = alpha_row.shape[1]
    src, lane = iota((2 * probes, AUX), 0), iota((2 * probes, AUX), 1)
    scale = 1.0 / (4 * probes)
    swapped = jnp.where(src < probes, src + probes, src - probes)
    pick = jnp.where(lane == src, 1.0, 0.0) + jnp.where(lane - 64 == swapped, -scale, 0.0)
    aux = lax.dot_general(probe_t, pick.astype(BF), TN, preferred_element_type=F32)
    spread = jnp.broadcast_to(alpha_row.astype(F32), (points, points))
    diag = jnp.where(iota((points, points), 0) == iota((points, points), 1), spread, 0.0)
    lane = iota((points, AUX), 1)
    put = jnp.where(lane == 2 * probes, 1.0, 0.0) + jnp.where(lane == 64 + 2 * probes, 0.5, 0.0)
    aux = aux + jnp.dot(diag.astype(BF), put.astype(BF), preferred_element_type=F32)
    return aux


def norms_of(feats):
    f = feats.astype(F32)
    return jnp.sum(f * f, axis=1, keepdims=True)


def with_norms(factors, norms):
    lane = iota(factors.shape, 1)
    for k in range(3):
        part = norms.astype(BF).astype(F32)
        factors = jnp.where(lane == 100 + k, part, factors)
        norms = norms - part
    return factors


def kernel(
    probes,
    amp_ref,
    lsq_ref,
    hidden_hbm,
    proj_hbm,
    alpha_hbm,
    probe_hbm,
    gh_ref,
    gp_ref,
    rows,
    row_feat,
    cols,
    left,
    bias,
    moved,
    rsum,
    sbuf,
    rplus,
    rminus,
    terms,
    pbuf,
    xrec,
    prec,
    zbuf,
    zrec,
    fbuf,
    frec,
    row_send,
    row_recv,
    col_send,
    col_recv,
    part_send,
    part_recv,
    rs_send,
    rs_recv,
    pair_send,
    pair_recv,
    p_send,
    p_recv,
    z_send,
    z_recv,
    f_send,
    f_recv,
    proj_ref,
    alpha_ref,
    probe_ref,
    in_sem,
):
    pts, hid = hidden_hbm.shape
    feat = proj_ref.shape[1]
    width = feat + AUX
    quarter, piece, row_piece = pts // 4, pts // PARTS, pts // ROW_PARTS
    m = 2 * pts

    r, c = lax.axis_index("row"), lax.axis_index("col")
    k, z, y_hi = r % 2, (r // 2) % NZ, r // (2 * NZ)
    x, y_lo = c // 2, c % 2
    y = y_hi * 2 + y_lo

    def dev(dx, dy, dz, flip=0):
        xx, yy, zz = (x + dx) % NX, (y + dy) % NY, (z + dz) % NZ
        kk = (1 - k) if flip else k
        return (((yy // 2) * NZ + zz) * 2 + kk, xx * 2 + yy % 2)

    plane = (dev(-1, 0, 0), dev(1, 0, 0), dev(0, -1, 0), dev(0, 1, 0))
    line = (dev(0, 0, -1), dev(0, 0, 1))
    partner = dev(0, 0, 0, 1)

    own_rows = pl.ds(POS[0] * pts, pts)
    hidden_ref = rows.at[own_rows, pl.ds(0, hid)]
    loads = [
        pltpu.make_async_copy(src, dst, in_sem.at[i])
        for i, (src, dst) in enumerate(
            (
                (hidden_hbm, hidden_ref),
                (alpha_hbm, alpha_ref),
                (probe_hbm, probe_ref),
                (proj_hbm, proj_ref),
            )
        )
    ]
    for load in loads:
        load.start()

    barrier = pltpu.get_barrier_semaphore()
    for peer in (*plane, *line, partner):
        pl.semaphore_signal(barrier, inc=1, device_id=peer, device_id_type=MESH)

    for load in loads[1:3]:
        load.wait()
    factors = factor_block(alpha_ref[...], probe_ref[...], probes)
    rows[own_rows, hid : hid + AUX] = factors.astype(BF)
    loads[0].wait()

    pl.semaphore_wait(barrier, 7)

    sends = []
    used = {}

    def send(src, dst, sems, recv_sem, to):
        if isinstance(sems, tuple):
            sem = sems[0].at[sems[1:]]
        else:
            sem = sems.at[used.setdefault(id(sems), 0)]
            used[id(sems)] += 1
        copy = pltpu.make_async_remote_copy(
            src_ref=src,
            dst_ref=dst,
            send_sem=sem,
            recv_sem=recv_sem,
            device_id=to,
            device_id_type=MESH,
        )
        copy.start()
        sends.append(copy)

    def arrived(dst, recv_sem):
        pltpu.make_async_remote_copy(
            src_ref=dst,
            dst_ref=dst,
            send_sem=recv_sem,
            recv_sem=recv_sem,
            device_id=partner,
            device_id_type=MESH,
        ).wait_recv()

    def row_part(d, q):
        return rows.at[pl.ds(POS[d] * pts + q * row_piece, row_piece), :]

    def col_part(core, dx, dy, q, n):
        start = SLOTS.index((core, dx, dy)) * pts + q * quarter
        return cols.at[pl.ds(start, n * quarter), :]

    scale = math.log2(math.e) / lsq_ref[0]
    final = 2.0 * amp_ref[0] / lsq_ref[0]
    lane16 = iota((16, AUX), 1)
    picks = jnp.where((lane16 >= 100) & (lane16 < 103), 1.0, 0.0).astype(BF)

    def prepare(g):
        rs = pl.ds(g * m, m)
        feats = jnp.dot(rows[rs, 0:hid], proj_ref[...], preferred_element_type=F32).astype(BF)
        row_feat[rs, :] = feats
        bias[rs, :] = norms_of(feats) * (-0.5 * scale)
        lane = iota((m, AUX), 1)
        raw = rows[rs, hid : hid + AUX].astype(F32)
        turned = pltpu.roll(raw, 64, 1)
        factors = jnp.where((lane >= 64) & (lane <= 64 + 2 * probes), turned, 0.0)
        left[rs, :] = factors.astype(BF)

    def chunk(g, first, n, fresh):
        rs, count = pl.ds(g * m, m), n * CHUNK
        cs = pl.ds(first * CHUNK, count)
        col_f = cols[cs, 0:feat]
        col_a = cols[cs, feat:width]
        sq = lax.dot_general(picks, col_a, NT, preferred_element_type=F32)[0:1, :]
        inner = lax.dot_general(row_feat[rs, :], col_f, NT, preferred_element_type=F32)
        gmat = lax.dot_general(left[rs, :], col_a, NT, preferred_element_type=F32)
        expo = inner * scale + (bias[rs, :] + sq * (-0.5 * scale))
        weight = gmat * jnp.exp2(expo)
        total = weight[:, :128]
        for t in range(1, count // 128):
            total = total + weight[:, t * 128 : (t + 1) * 128]
        term = jnp.dot(weight.astype(BF), col_f, preferred_element_type=F32)
        if fresh:
            rsum[rs, :] = total
            moved[rs, :] = term
        else:
            rsum[rs, :] += total
            moved[rs, :] += term

    def finish(g, fresh, last):
        rs = pl.ds(g * m, m)
        rowsum = jnp.sum(rsum[rs, :], axis=1, keepdims=True)
        value = moved[rs, :] - rowsum * row_feat[rs, :].astype(F32)
        moved[rs, :] = value
        term = lax.dot_general(rows[rs, 0:hid], value.astype(BF), TN, preferred_element_type=F32)
        if last:
            pbuf[...] = ((terms[...] + term) * final).astype(BF).reshape(pbuf.shape)
        else:
            terms[...] = term if fresh else terms[...] + term

    def pass_on(d, i):
        up = d < 4 or (d == 4 and i < PARTS // 2)
        dst, way = (rplus, 0) if up else (rminus, 1)
        step = 4 - d if up else d - 4
        rs = pl.ds(POS[d] * pts + i * piece, piece)
        ps = pl.ds(i * piece, piece)
        value = moved[rs, :]
        if step > 1 or (step == 1 and up == (i < PARTS // 2)):
            arrived(dst.at[step - 1, ps, :], rs_recv.at[way, step - 1, i])
            value = value + dst[step - 1, ps, :].astype(F32)
        sbuf[rs, :] = value.astype(BF)
        send(sbuf.at[rs, :], dst.at[step, ps, :], rs_send, rs_recv.at[way, step, i], line[up])

    def row_step(op):
        if op[0] == "wr":
            arrived(row_part(*op[1:]), row_recv.at[op[1:]])
        else:
            d, q, to_d, up = op[1:]
            send(row_part(d, q), row_part(to_d, q), row_send, row_recv.at[to_d, q], line[up])

    def col_step(op):
        if op[0] == "wc":
            arrived(col_part(0, *op[1:], 1), col_recv.at[op[1:]])
        elif op[0] == "c":
            dx, dy, q, to_dx, to_dy, way = op[1:]
            dst = col_part(0, to_dx, to_dy, q, 1)
            send(col_part(0, dx, dy, q, 1), dst, col_send, col_recv.at[to_dx, to_dy, q], plane[way])
        else:
            dx, dy, h = op[1:]
            dst = col_part(1, dx, dy, 2 * h, 2)
            if op[0] == "wp":
                arrived(dst, part_recv.at[dx, dy, h])
            else:
                src = col_part(0, dx, dy, 2 * h, 2)
                send(src, dst, part_send, part_recv.at[dx, dy, h], partner)

    at = 0
    while PLAN[at][0] == "r":
        row_step(PLAN[at])
        at += 1
    loads[3].wait()
    feats = jnp.dot(hidden_ref[...], proj_ref[...], preferred_element_type=F32).astype(BF)
    own = pl.ds(SLOTS.index((0, 0, 0)) * pts, pts)
    cols[own, 0:feat] = feats
    cols[own, feat:width] = with_norms(factors, norms_of(feats)).astype(BF)

    seen, finished = set(), 0
    while finished < GROUPS:
        op = PLAN[at]
        at += 1
        if op[0] == "G":
            prepare(op[1])
        elif op[0] == "g":
            g, j = op[1:]
            n = 1
            while n < MERGE and PLAN[at] == ("g", g, j + n):
                at, n = at + 1, n + 1
            chunk(g, j, n, g not in seen)
            seen.add(g)
        elif op[0] == "F":
            finish(op[1], finished == 0, finished == GROUPS - 1)
            finished += 1
        elif op[0] == "R":
            pass_on(*op[1:])
        elif op[0] in ("r", "wr"):
            row_step(op)
        else:
            col_step(op)

    send(pbuf.at[:, :, 1 - k], xrec, (pair_send, 0), pair_recv.at[0], partner)
    arrived(xrec, pair_recv.at[0])
    pbuf[:, :, k] = (pbuf[:, :, k].astype(F32) + xrec[...].astype(F32)).astype(BF)

    def portion(xx, yy):
        lanes = pl.ds(pl.multiple_of(xx * 128, 128), 128)
        return yy // 2, yy % 2, k, slice(None), slice(None), lanes

    for dx in (2, 1, 3, 0):
        for dy in (2, 1, 3, 0):
            if dx or dy:
                to = ((NX - dx) % NX, (NY - dy) % NY)
                send(
                    pbuf.at[portion((x + dx) % NX, (y + dy) % NY)],
                    prec.at[to[0], to[1]],
                    (p_send, dx, dy),
                    p_recv.at[to[0], to[1]],
                    dev(dx, dy, 0),
                )

    for op in PLAN[at : len(PLAN) - LATE]:
        pass_on(*op[1:])
    share = pbuf[portion(x, y)].astype(F32)
    for dx in range(NX):
        for dy in range(NY):
            if dx or dy:
                arrived(prec.at[dx, dy], p_recv.at[dx, dy])
                share = share + prec[dx, dy].astype(F32)
    zbuf[...] = share.astype(BF)

    def falls_here(zz):
        return (zz // 4 == y_lo) & (zz % 4 // 2 == k)

    gathers = falls_here(z)
    later = []

    def send_if(cond, src, dst, send_sem, recv_sem, to):
        copy = pltpu.make_async_remote_copy(
            src_ref=src,
            dst_ref=dst,
            send_sem=send_sem,
            recv_sem=recv_sem,
            device_id=to,
            device_id_type=MESH,
        )

        @pl.when(cond)
        def _():
            copy.start()

        later.append((cond, copy))

    for dz in (4, 3, 5, 2, 6, 1, 7):
        zz = (z + dz) % NZ
        send_if(
            falls_here(zz),
            zbuf.at[zz % 2],
            zrec.at[NZ - dz],
            z_send.at[dz],
            z_recv.at[NZ - dz],
            dev(0, 0, dz),
        )

    for op in PLAN[len(PLAN) - LATE :]:
        pass_on(*op[1:])
    for i in range(PARTS):
        ps = pl.ds(i * piece, piece)
        arrived(rplus.at[3, ps, :], rs_recv.at[0, 3, i])
        arrived(rminus.at[3, ps, :], rs_recv.at[1, 3, i])
    total = moved[0:pts, :] + rplus[3].astype(F32) + rminus[3].astype(F32)
    grad = (total * final).astype(BF)
    gh_ref[...] = lax.dot_general(grad, proj_ref[...], NT, preferred_element_type=F32).astype(BF)

    @pl.when(gathers)
    def _():
        total = zbuf[z % 2].astype(F32)
        for dz in range(1, NZ):
            arrived(zrec.at[dz], z_recv.at[dz])
            total = total + zrec[dz].astype(F32)
        fbuf[...] = total.reshape(fbuf.shape).astype(BF)

    for flip in (1, 0):
        for dx in (2, 1, 3, 0):
            for core in range(2):
                xx, yy = (x + dx) % NX, (y_lo if flip == 0 else 1 - y_lo)
                to = ((y_hi * NZ + z) * 2 + core, xx * 2 + yy)
                slot = (NX - dx) % NX
                send_if(
                    gathers if dx or flip else gathers & (k != core),
                    fbuf.at[core],
                    frec.at[slot],
                    f_send.at[dx, flip, core],
                    f_recv.at[slot],
                    to,
                )

    @pl.when(gathers)
    def _():
        frec[0] = fbuf[k]

    for dx in range(NX):
        if dx == 0:

            @pl.when(jnp.logical_not(gathers))
            def _():
                arrived(frec.at[0], f_recv.at[0])

        else:
            arrived(frec.at[dx], f_recv.at[dx])
        gp_ref[:, pl.ds(pl.multiple_of((x + dx) % NX * 128, 128), 128)] = frec[dx].astype(F32)

    for copy in sends:
        copy.wait_send()
    for cond, copy in later:

        @pl.when(cond)
        def _():
            copy.wait_send()


def fused(hidden, projection, alpha, probe_pairs, amplitude, length_sq):
    pts, hid = hidden.shape
    feat = projection.shape[1]
    probes = probe_pairs.shape[1] // 2
    width = feat + AUX
    n_rows, n_cols = NZ * pts, 2 * NX * NY * pts
    size = hid // (4 * NZ)
    arrays = (hidden, projection, alpha[None, :], probe_pairs.T)
    vmem = pl.BlockSpec(memory_space=pltpu.VMEM)
    hbm = pl.BlockSpec(memory_space=pltpu.HBM)
    smem = pl.BlockSpec(memory_space=pltpu.SMEM)
    dma = pltpu.SemaphoreType.DMA
    return pl.pallas_call(
        functools.partial(kernel, probes),
        out_shape=(
            jax.ShapeDtypeStruct((pts, hid), BF),
            jax.ShapeDtypeStruct((hid // (4 * NZ), feat), F32),
        ),
        in_specs=[smem, smem, hbm, hbm, hbm, hbm],
        out_specs=(vmem, vmem),
        scratch_shapes=[
            pltpu.VMEM((n_rows, hid + AUX), BF),
            pltpu.VMEM((n_rows, feat), BF),
            pltpu.VMEM((n_cols, width), BF),
            pltpu.VMEM((n_rows, AUX), BF),
            pltpu.VMEM((n_rows, 1), F32),
            pltpu.VMEM((n_rows, feat), F32),
            pltpu.VMEM((n_rows, 128), F32),
            pltpu.VMEM((n_rows, feat), BF),
            pltpu.VMEM((4, pts, feat), BF),
            pltpu.VMEM((4, pts, feat), BF),
            pltpu.VMEM((hid, feat), F32),
            pltpu.VMEM((2, 2, 2, 2, 2 * size, feat), BF),
            pltpu.VMEM((2, 2, 2, 2 * size, feat), BF),
            pltpu.VMEM((NX, NY, 2, 2 * size, 128), BF),
            pltpu.VMEM((2, 2 * size, 128), BF),
            pltpu.VMEM((NZ, 2 * size, 128), BF),
            pltpu.VMEM((2, size, 128), BF),
            pltpu.VMEM((NX, size, 128), BF),
            dma((7 * ROW_PARTS,)),
            dma((NZ, ROW_PARTS)),
            dma((60,)),
            dma((NX, NY, 4)),
            dma((32,)),
            dma((NX, NY, 2)),
            dma((7 * PARTS,)),
            dma((2, 4, PARTS)),
            dma((1,)),
            dma((1,)),
            dma((NX, NY)),
            dma((NX, NY)),
            dma((NZ,)),
            dma((NZ,)),
            dma((NX, 2, 2)),
            dma((NX,)),
            pltpu.VMEM((hid, feat), BF),
            pltpu.VMEM((1, pts), BF),
            pltpu.VMEM((2 * probes, pts), BF),
            dma((4,)),
        ],
        compiler_params=pltpu.CompilerParams(
            collective_id=0, has_side_effects=True, vmem_limit_bytes=28 << 20
        ),
        name="fused",
    )(amplitude, length_sq, *(pltpu.with_memory_space_constraint(a, pltpu.HBM) for a in arrays))


def per_device(hidden, projection, alpha, probe_pairs, amplitude, length_sq):
    return fused(hidden, projection, alpha, probe_pairs, amplitude, length_sq)


def solution(mesh):
    placed = (P(("row", "col"), None), P(), P(("row", "col")), P(("row", "col"), None), P(), P())
    return jax.shard_map(
        per_device,
        mesh=mesh,
        in_specs=placed,
        out_specs=(P(("row", "col"), None), P("row", None)),
        check_vma=False,
    )
```

```python
import functools
import math

import jax
import jax.numpy as jnp
from jax import lax
from jax.experimental import pallas as pl
from jax.experimental.pallas import tpu as pltpu
from jax.sharding import PartitionSpec as P

MESH = pl.DeviceIdType.MESH
NT = (((1,), (1,)), ((), ()))
TN = (((0,), (0,)), ((), ()))
BF, F32 = jnp.bfloat16, jnp.float32

NX, NY, NZ = 4, 4, 8
AUX = 128
POS = {0: 0, 4: 1, 3: 2, 5: 3, 2: 4, 6: 5, 1: 6, 7: 7}
GROUPS = 4
CHUNK = 1024
MERGE = 2
EARLY = 4
LATE = 0
PARTS = 4
ROW_PARTS = 4
SLOTS = [
    (0, 0, 0), (1, 0, 0), (0, 0, 1), (0, 0, 3), (0, 1, 0), (0, 3, 0), (1, 0, 1), (1, 0, 3),
    (1, 1, 0), (1, 3, 0), (0, 1, 1), (0, 1, 3), (0, 3, 1), (0, 3, 3), (1, 1, 1), (0, 0, 2),
    (0, 2, 0), (1, 1, 3), (1, 3, 1), (1, 3, 3), (1, 0, 2), (1, 2, 0), (0, 1, 2), (0, 2, 1),
    (0, 2, 3), (0, 3, 2), (1, 1, 2), (1, 2, 1), (1, 2, 3), (1, 3, 2), (0, 2, 2), (1, 2, 2),
]
PLAN = [
    ("r", 0, 0, 1, 0), ("r", 0, 0, 7, 1), ("r", 0, 1, 1, 0), ("r", 0, 1, 7, 1), ("r", 0, 2, 1, 0), ("r", 0, 2, 7, 1),
    ("r", 0, 3, 1, 0), ("r", 0, 3, 7, 1), ("c", 0, 0, 0, 1, 0, 0), ("c", 0, 0, 1, 1, 0, 0), ("c", 0, 0, 2, 0, 1, 2),
    ("c", 0, 0, 3, 0, 1, 2), ("c", 0, 0, 0, 3, 0, 1), ("c", 0, 0, 1, 3, 0, 1), ("c", 0, 0, 2, 0, 3, 3),
    ("c", 0, 0, 3, 0, 3, 3), ("c", 0, 0, 0, 0, 1, 2), ("c", 0, 0, 1, 0, 1, 2), ("c", 0, 0, 2, 1, 0, 0),
    ("c", 0, 0, 3, 1, 0, 0), ("c", 0, 0, 0, 0, 3, 3), ("c", 0, 0, 1, 0, 3, 3), ("c", 0, 0, 2, 3, 0, 1),
    ("c", 0, 0, 3, 3, 0, 1), ("p", 0, 0, 0), ("p", 0, 0, 1), ("wp", 0, 0, 0), ("wp", 0, 0, 1), ("wr", 1, 0),
    ("r", 1, 0, 2, 0), ("wr", 7, 0), ("r", 7, 0, 6, 1), ("wc", 0, 1, 2), ("c", 0, 1, 2, 0, 2, 2),
    ("c", 0, 1, 2, 1, 1, 0), ("c", 0, 1, 2, 3, 1, 1), ("wc", 0, 3, 2), ("c", 0, 3, 2, 1, 3, 0),
    ("c", 0, 3, 2, 3, 3, 1), ("wc", 1, 0, 0), ("c", 1, 0, 0, 2, 0, 0), ("c", 1, 0, 0, 1, 1, 2),
    ("c", 1, 0, 0, 1, 3, 3), ("wc", 3, 0, 0), ("c", 3, 0, 0, 3, 1, 2), ("c", 3, 0, 0, 3, 3, 3), ("wc", 0, 1, 3),
    ("c", 0, 1, 3, 1, 1, 0), ("c", 0, 1, 3, 3, 1, 1), ("p", 0, 1, 1), ("wc", 0, 3, 3), ("c", 0, 3, 3, 0, 2, 3),
    ("c", 0, 3, 3, 1, 3, 0), ("c", 0, 3, 3, 3, 3, 1), ("p", 0, 3, 1), ("wc", 1, 0, 1), ("c", 1, 0, 1, 1, 1, 2),
    ("c", 1, 0, 1, 1, 3, 3), ("p", 1, 0, 0), ("wc", 3, 0, 1), ("c", 3, 0, 1, 2, 0, 1), ("c", 3, 0, 1, 3, 1, 2),
    ("c", 3, 0, 1, 3, 3, 3), ("p", 3, 0, 0), ("wr", 1, 1), ("r", 1, 1, 2, 0), ("wr", 7, 1), ("r", 7, 1, 6, 1),
    ("wc", 0, 1, 0), ("c", 0, 1, 0, 0, 2, 2), ("wc", 0, 3, 0), ("wc", 1, 0, 2), ("c", 1, 0, 2, 2, 0, 0),
    ("wc", 3, 0, 2), ("wp", 0, 1, 1), ("wr", 1, 2), ("r", 1, 2, 2, 0), ("wr", 7, 2), ("r", 7, 2, 6, 1),
    ("wp", 0, 3, 1), ("wc", 0, 1, 1), ("p", 0, 1, 0), ("wc", 0, 3, 1), ("c", 0, 3, 1, 0, 2, 3), ("p", 0, 3, 0),
    ("wc", 1, 0, 3), ("p", 1, 0, 1), ("wc", 3, 0, 3), ("c", 3, 0, 3, 2, 0, 1), ("p", 3, 0, 1), ("wp", 1, 0, 0),
    ("wp", 3, 0, 0), ("wr", 1, 3), ("r", 1, 3, 2, 0), ("wr", 7, 3), ("r", 7, 3, 6, 1), ("wc", 0, 2, 2),
    ("c", 0, 2, 2, 1, 2, 0), ("c", 0, 2, 2, 3, 2, 1), ("wc", 1, 1, 2), ("c", 1, 1, 2, 2, 1, 0), ("wc", 1, 3, 0),
    ("wc", 3, 1, 2), ("wp", 0, 1, 0), ("wp", 0, 3, 0), ("G", 3), ("g", 3, 0), ("wr", 2, 0), ("r", 2, 0, 3, 0),
    ("wr", 6, 0), ("r", 6, 0, 5, 1), ("wc", 0, 2, 3), ("c", 0, 2, 3, 1, 2, 0), ("c", 0, 2, 3, 3, 2, 1),
    ("p", 0, 2, 1), ("wc", 2, 0, 0), ("c", 2, 0, 0, 2, 1, 2), ("c", 2, 0, 0, 2, 3, 3), ("wc", 1, 1, 0),
    ("c", 1, 1, 0, 1, 2, 2), ("wc", 1, 3, 2), ("c", 1, 3, 2, 2, 3, 0), ("wc", 3, 3, 0), ("wc", 3, 3, 2),
    ("wc", 3, 1, 0), ("c", 3, 1, 0, 3, 2, 2), ("wc", 3, 1, 3), ("c", 3, 1, 3, 2, 1, 1), ("p", 3, 1, 1),
    ("wp", 1, 0, 1), ("wp", 3, 0, 1), ("wr", 2, 1), ("r", 2, 1, 3, 0), ("wr", 6, 1), ("r", 6, 1, 5, 1),
    ("wc", 1, 1, 1), ("p", 1, 1, 0), ("wc", 1, 1, 3), ("p", 1, 1, 1), ("wc", 1, 3, 1), ("c", 1, 3, 1, 1, 2, 3),
    ("p", 1, 3, 0), ("wc", 3, 3, 3), ("c", 3, 3, 3, 2, 3, 1), ("p", 3, 3, 1), ("wp", 0, 2, 1), ("wc", 2, 0, 1),
    ("c", 2, 0, 1, 2, 1, 2), ("c", 2, 0, 1, 2, 3, 3), ("p", 2, 0, 0), ("wc", 1, 3, 3), ("p", 1, 3, 1),
    ("wc", 3, 1, 1), ("p", 3, 1, 0), ("wc", 3, 3, 1), ("c", 3, 3, 1, 3, 2, 3), ("p", 3, 3, 0), ("wp", 3, 1, 1),
    ("wr", 2, 2), ("r", 2, 2, 3, 0), ("wr", 6, 2), ("r", 6, 2, 5, 1), ("wp", 1, 1, 0), ("wp", 1, 1, 1),
    ("wc", 0, 2, 0), ("wc", 0, 2, 1), ("p", 0, 2, 0), ("wc", 2, 0, 2), ("wc", 2, 0, 3), ("p", 2, 0, 1), ("g", 3, 1),
    ("wr", 2, 3), ("r", 2, 3, 3, 0), ("wr", 6, 3), ("r", 6, 3, 5, 1), ("wc", 1, 2, 2), ("c", 1, 2, 2, 2, 2, 0),
    ("wc", 3, 2, 2), ("wp", 1, 3, 0), ("wc", 2, 1, 0), ("c", 2, 1, 0, 2, 2, 2), ("wc", 2, 3, 0), ("wp", 3, 3, 1),
    ("wp", 2, 0, 0), ("wp", 1, 3, 1), ("G", 2), ("g", 2, 0), ("wr", 3, 0), ("r", 3, 0, 4, 0), ("wr", 5, 0),
    ("wc", 3, 2, 3), ("c", 3, 2, 3, 2, 2, 1), ("p", 3, 2, 1), ("wc", 2, 1, 2), ("wc", 1, 2, 0), ("wc", 1, 2, 1),
    ("p", 1, 2, 0), ("wp", 3, 1, 0), ("wp", 3, 3, 0), ("wp", 0, 2, 0), ("wp", 2, 0, 1), ("g", 2, 1), ("wr", 3, 1),
    ("r", 3, 1, 4, 0), ("wr", 5, 1), ("wc", 1, 2, 3), ("p", 1, 2, 1), ("wc", 2, 3, 1), ("c", 2, 3, 1, 2, 2, 3),
    ("p", 2, 3, 0), ("wc", 2, 1, 3), ("p", 2, 1, 1), ("wc", 3, 2, 0), ("wc", 2, 3, 2), ("wc", 2, 3, 3),
    ("p", 2, 3, 1), ("wc", 2, 1, 1), ("p", 2, 1, 0), ("wc", 3, 2, 1), ("p", 3, 2, 0), ("g", 2, 2), ("wr", 3, 2),
    ("wr", 5, 2), ("r", 5, 2, 4, 1), ("wc", 2, 2, 2), ("wc", 2, 2, 0), ("wp", 3, 2, 1), ("wp", 1, 2, 0), ("g", 3, 2),
    ("wr", 3, 3), ("wr", 5, 3), ("r", 5, 3, 4, 1), ("wp", 1, 2, 1), ("wp", 2, 3, 0), ("wp", 2, 1, 1), ("wp", 2, 3, 1),
    ("G", 1), ("g", 1, 0), ("wr", 4, 0), ("wc", 2, 2, 3), ("p", 2, 2, 1), ("wc", 2, 2, 1), ("p", 2, 2, 0),
    ("wp", 2, 1, 0), ("wp", 3, 2, 0), ("g", 1, 1), ("wr", 4, 1), ("g", 1, 2), ("wr", 4, 2), ("wp", 2, 2, 1),
    ("wp", 2, 2, 0), ("g", 1, 3), ("F", 1), ("wr", 4, 3), ("R", 3, 2), ("R", 3, 3), ("R", 5, 0), ("R", 5, 1),
    ("G", 0), ("g", 0, 0), ("g", 0, 1), ("g", 0, 2), ("g", 0, 3), ("F", 0), ("R", 4, 0), ("R", 4, 1), ("R", 4, 2),
    ("R", 4, 3), ("g", 2, 3), ("F", 2), ("R", 2, 2), ("R", 2, 3), ("R", 6, 0), ("R", 6, 1), ("g", 3, 3), ("F", 3),
    ("R", 3, 0), ("R", 5, 2), ("R", 3, 1), ("R", 5, 3), ("R", 1, 2), ("R", 7, 0), ("R", 1, 3), ("R", 7, 1),
    ("R", 2, 0), ("R", 6, 2), ("R", 2, 1), ("R", 6, 3), ("R", 1, 0), ("R", 7, 2), ("R", 1, 1), ("R", 7, 3),
]


def iota(shape, dim):
    return lax.broadcasted_iota(jnp.int32, shape, dim)


def factor_block(alpha_row, probe_t, probes):
    points = alpha_row.shape[1]
    src, lane = iota((2 * probes, AUX), 0), iota((2 * probes, AUX), 1)
    scale = 1.0 / (4 * probes)
    swapped = jnp.where(src < probes, src + probes, src - probes)
    pick = jnp.where(lane == src, 1.0, 0.0) + jnp.where(lane - 64 == swapped, -scale, 0.0)
    aux = lax.dot_general(probe_t, pick.astype(BF), TN, preferred_element_type=F32)
    spread = jnp.broadcast_to(alpha_row.astype(F32), (points, points))
    diag = jnp.where(iota((points, points), 0) == iota((points, points), 1), spread, 0.0)
    lane = iota((points, AUX), 1)
    put = jnp.where(lane == 2 * probes, 1.0, 0.0) + jnp.where(lane == 64 + 2 * probes, 0.5, 0.0)
    aux = aux + jnp.dot(diag.astype(BF), put.astype(BF), preferred_element_type=F32)
    return aux


def norms_of(feats):
    f = feats.astype(F32)
    return jnp.sum(f * f, axis=1, keepdims=True)


def with_norms(factors, norms):
    lane = iota(factors.shape, 1)
    for k in range(3):
        part = norms.astype(BF).astype(F32)
        factors = jnp.where(lane == 100 + k, part, factors)
        norms = norms - part
    return factors


def kernel(
    probes,
    amp_ref,
    lsq_ref,
    hidden_hbm,
    proj_hbm,
    alpha_hbm,
    probe_hbm,
    gh_ref,
    gp_ref,
    rows,
    row_feat,
    cols,
    left,
    bias,
    moved,
    rsum,
    sbuf,
    rplus,
    rminus,
    terms,
    pbuf,
    xrec,
    prec,
    zbuf,
    zrec,
    fbuf,
    frec,
    row_send,
    row_recv,
    col_send,
    col_recv,
    part_send,
    part_recv,
    rs_send,
    rs_recv,
    pair_send,
    pair_recv,
    p_send,
    p_recv,
    z_send,
    z_recv,
    f_send,
    f_recv,
    proj_ref,
    alpha_ref,
    probe_ref,
    in_sem,
):
    pts, hid = hidden_hbm.shape
    feat = proj_ref.shape[1]
    width = feat + AUX
    quarter, piece, row_piece = pts // 4, pts // PARTS, pts // ROW_PARTS
    m = 2 * pts

    r, c = lax.axis_index("row"), lax.axis_index("col")
    k, z, y_hi = r % 2, (r // 2) % NZ, r // (2 * NZ)
    x, y_lo = c // 2, c % 2
    y = y_hi * 2 + y_lo

    def dev(dx, dy, dz, flip=0):
        xx, yy, zz = (x + dx) % NX, (y + dy) % NY, (z + dz) % NZ
        kk = (1 - k) if flip else k
        return (((yy // 2) * NZ + zz) * 2 + kk, xx * 2 + yy % 2)

    plane = (dev(-1, 0, 0), dev(1, 0, 0), dev(0, -1, 0), dev(0, 1, 0))
    line = (dev(0, 0, -1), dev(0, 0, 1))
    partner = dev(0, 0, 0, 1)

    own_rows = pl.ds(POS[0] * pts, pts)
    hidden_ref = rows.at[own_rows, pl.ds(0, hid)]
    loads = [
        pltpu.make_async_copy(src, dst, in_sem.at[i])
        for i, (src, dst) in enumerate(
            (
                (hidden_hbm, hidden_ref),
                (alpha_hbm, alpha_ref),
                (probe_hbm, probe_ref),
                (proj_hbm, proj_ref),
            )
        )
    ]
    for load in loads:
        load.start()

    barrier = pltpu.get_barrier_semaphore()
    for peer in (*plane, *line, partner):
        pl.semaphore_signal(barrier, inc=1, device_id=peer, device_id_type=MESH)

    for load in loads[1:3]:
        load.wait()
    factors = factor_block(alpha_ref[...], probe_ref[...], probes)
    rows[own_rows, hid : hid + AUX] = factors.astype(BF)
    loads[0].wait()

    pl.semaphore_wait(barrier, 7)

    sends = []
    used = {}

    def send(src, dst, sems, recv_sem, to):
        if isinstance(sems, tuple):
            sem = sems[0].at[sems[1:]]
        else:
            sem = sems.at[used.setdefault(id(sems), 0)]
            used[id(sems)] += 1
        copy = pltpu.make_async_remote_copy(
            src_ref=src,
            dst_ref=dst,
            send_sem=sem,
            recv_sem=recv_sem,
            device_id=to,
            device_id_type=MESH,
        )
        copy.start()
        sends.append(copy)

    def arrived(dst, recv_sem):
        pltpu.make_async_remote_copy(
            src_ref=dst,
            dst_ref=dst,
            send_sem=recv_sem,
            recv_sem=recv_sem,
            device_id=partner,
            device_id_type=MESH,
        ).wait_recv()

    def row_part(d, q):
        return rows.at[pl.ds(POS[d] * pts + q * row_piece, row_piece), :]

    def col_part(core, dx, dy, q, n):
        start = SLOTS.index((core, dx, dy)) * pts + q * quarter
        return cols.at[pl.ds(start, n * quarter), :]

    scale = math.log2(math.e) / lsq_ref[0]
    final = 2.0 * amp_ref[0] / lsq_ref[0]
    lane16 = iota((16, AUX), 1)
    picks = jnp.where((lane16 >= 100) & (lane16 < 103), 1.0, 0.0).astype(BF)

    def prepare(g):
        rs = pl.ds(g * m, m)
        feats = jnp.dot(rows[rs, 0:hid], proj_ref[...], preferred_element_type=F32).astype(BF)
        row_feat[rs, :] = feats
        bias[rs, :] = norms_of(feats) * (-0.5 * scale)
        lane = iota((m, AUX), 1)
        raw = rows[rs, hid : hid + AUX].astype(F32)
        turned = pltpu.roll(raw, 64, 1)
        factors = jnp.where((lane >= 64) & (lane <= 64 + 2 * probes), turned, 0.0)
        left[rs, :] = factors.astype(BF)

    def chunk(g, first, n, fresh):
        rs, count = pl.ds(g * m, m), n * CHUNK
        cs = pl.ds(first * CHUNK, count)
        col_f = cols[cs, 0:feat]
        col_a = cols[cs, feat:width]
        sq = lax.dot_general(picks, col_a, NT, preferred_element_type=F32)[0:1, :]
        inner = lax.dot_general(row_feat[rs, :], col_f, NT, preferred_element_type=F32)
        gmat = lax.dot_general(left[rs, :], col_a, NT, preferred_element_type=F32)
        expo = inner * scale + (bias[rs, :] + sq * (-0.5 * scale))
        weight = gmat * jnp.exp2(expo)
        total = weight[:, :128]
        for t in range(1, count // 128):
            total = total + weight[:, t * 128 : (t + 1) * 128]
        term = jnp.dot(weight.astype(BF), col_f, preferred_element_type=F32)
        if fresh:
            rsum[rs, :] = total
            moved[rs, :] = term
        else:
            rsum[rs, :] += total
            moved[rs, :] += term

    def finish(g, fresh, last):
        rs = pl.ds(g * m, m)
        rowsum = jnp.sum(rsum[rs, :], axis=1, keepdims=True)
        value = moved[rs, :] - rowsum * row_feat[rs, :].astype(F32)
        moved[rs, :] = value
        term = lax.dot_general(rows[rs, 0:hid], value.astype(BF), TN, preferred_element_type=F32)
        if last:
            pbuf[...] = ((terms[...] + term) * final).astype(BF).reshape(pbuf.shape)
        else:
            terms[...] = term if fresh else terms[...] + term

    def pass_on(d, i):
        up = d < 4 or (d == 4 and i < PARTS // 2)
        dst, way = (rplus, 0) if up else (rminus, 1)
        step = 4 - d if up else d - 4
        rs = pl.ds(POS[d] * pts + i * piece, piece)
        ps = pl.ds(i * piece, piece)
        value = moved[rs, :]
        if step > 1 or (step == 1 and up == (i < PARTS // 2)):
            arrived(dst.at[step - 1, ps, :], rs_recv.at[way, step - 1, i])
            value = value + dst[step - 1, ps, :].astype(F32)
        sbuf[rs, :] = value.astype(BF)
        send(sbuf.at[rs, :], dst.at[step, ps, :], rs_send, rs_recv.at[way, step, i], line[up])

    def row_step(op):
        if op[0] == "wr":
            arrived(row_part(*op[1:]), row_recv.at[op[1:]])
        else:
            d, q, to_d, up = op[1:]
            send(row_part(d, q), row_part(to_d, q), row_send, row_recv.at[to_d, q], line[up])

    def col_step(op):
        if op[0] == "wc":
            arrived(col_part(0, *op[1:], 1), col_recv.at[op[1:]])
        elif op[0] == "c":
            dx, dy, q, to_dx, to_dy, way = op[1:]
            dst = col_part(0, to_dx, to_dy, q, 1)
            send(col_part(0, dx, dy, q, 1), dst, col_send, col_recv.at[to_dx, to_dy, q], plane[way])
        else:
            dx, dy, h = op[1:]
            dst = col_part(1, dx, dy, 2 * h, 2)
            if op[0] == "wp":
                arrived(dst, part_recv.at[dx, dy, h])
            else:
                src = col_part(0, dx, dy, 2 * h, 2)
                send(src, dst, part_send, part_recv.at[dx, dy, h], partner)

    at = 0
    while PLAN[at][0] == "r":
        row_step(PLAN[at])
        at += 1
    loads[3].wait()
    feats = jnp.dot(hidden_ref[...], proj_ref[...], preferred_element_type=F32).astype(BF)
    own = pl.ds(SLOTS.index((0, 0, 0)) * pts, pts)
    cols[own, 0:feat] = feats
    cols[own, feat:width] = with_norms(factors, norms_of(feats)).astype(BF)

    seen, finished = set(), 0
    while finished < GROUPS:
        op = PLAN[at]
        at += 1
        if op[0] == "G":
            prepare(op[1])
        elif op[0] == "g":
            g, j = op[1:]
            n = 1
            while n < MERGE and PLAN[at] == ("g", g, j + n):
                at, n = at + 1, n + 1
            chunk(g, j, n, g not in seen)
            seen.add(g)
        elif op[0] == "F":
            finish(op[1], finished == 0, finished == GROUPS - 1)
            finished += 1
        elif op[0] == "R":
            pass_on(*op[1:])
        elif op[0] in ("r", "wr"):
            row_step(op)
        else:
            col_step(op)

    send(pbuf.at[:, :, 1 - k], xrec, (pair_send, 0), pair_recv.at[0], partner)
    for op in PLAN[at : at + EARLY]:
        pass_on(*op[1:])
    at += EARLY
    arrived(xrec, pair_recv.at[0])
    pbuf[:, :, k] = (pbuf[:, :, k].astype(F32) + xrec[...].astype(F32)).astype(BF)

    def portion(xx, yy):
        lanes = pl.ds(pl.multiple_of(xx * 128, 128), 128)
        return yy // 2, yy % 2, k, slice(None), slice(None), lanes

    for dx in (2, 1, 3, 0):
        for dy in (2, 1, 3, 0):
            if dx or dy:
                to = ((NX - dx) % NX, (NY - dy) % NY)
                send(
                    pbuf.at[portion((x + dx) % NX, (y + dy) % NY)],
                    prec.at[to[0], to[1]],
                    (p_send, dx, dy),
                    p_recv.at[to[0], to[1]],
                    dev(dx, dy, 0),
                )

    for op in PLAN[at : len(PLAN) - LATE]:
        pass_on(*op[1:])
    share = pbuf[portion(x, y)].astype(F32)
    for dx in range(NX):
        for dy in range(NY):
            if dx or dy:
                arrived(prec.at[dx, dy], p_recv.at[dx, dy])
                share = share + prec[dx, dy].astype(F32)
    zbuf[...] = share.astype(BF)

    def falls_here(zz):
        return (zz // 4 == y_lo) & (zz % 4 // 2 == k)

    gathers = falls_here(z)
    later = []

    def send_if(cond, src, dst, send_sem, recv_sem, to):
        copy = pltpu.make_async_remote_copy(
            src_ref=src,
            dst_ref=dst,
            send_sem=send_sem,
            recv_sem=recv_sem,
            device_id=to,
            device_id_type=MESH,
        )

        @pl.when(cond)
        def _():
            copy.start()

        later.append((cond, copy))

    for dz in (4, 3, 5, 2, 6, 1, 7):
        zz = (z + dz) % NZ
        send_if(
            falls_here(zz),
            zbuf.at[zz % 2],
            zrec.at[NZ - dz],
            z_send.at[dz],
            z_recv.at[NZ - dz],
            dev(0, 0, dz),
        )

    for op in PLAN[len(PLAN) - LATE :]:
        pass_on(*op[1:])
    for i in range(PARTS):
        ps = pl.ds(i * piece, piece)
        arrived(rplus.at[3, ps, :], rs_recv.at[0, 3, i])
        arrived(rminus.at[3, ps, :], rs_recv.at[1, 3, i])
    total = moved[0:pts, :] + rplus[3].astype(F32) + rminus[3].astype(F32)
    grad = (total * final).astype(BF)
    gh_ref[...] = lax.dot_general(grad, proj_ref[...], NT, preferred_element_type=F32).astype(BF)

    @pl.when(gathers)
    def _():
        total = zbuf[z % 2].astype(F32)
        for dz in range(1, NZ):
            arrived(zrec.at[dz], z_recv.at[dz])
            total = total + zrec[dz].astype(F32)
        fbuf[...] = total.reshape(fbuf.shape).astype(BF)

    for flip in (1, 0):
        for dx in (2, 1, 3, 0):
            for core in range(2):
                xx, yy = (x + dx) % NX, (y_lo if flip == 0 else 1 - y_lo)
                to = ((y_hi * NZ + z) * 2 + core, xx * 2 + yy)
                slot = (NX - dx) % NX
                send_if(
                    gathers if dx or flip else gathers & (k != core),
                    fbuf.at[core],
                    frec.at[slot],
                    f_send.at[dx, flip, core],
                    f_recv.at[slot],
                    to,
                )

    @pl.when(gathers)
    def _():
        frec[0] = fbuf[k]

    for dx in range(NX):
        if dx == 0:

            @pl.when(jnp.logical_not(gathers))
            def _():
                arrived(frec.at[0], f_recv.at[0])

        else:
            arrived(frec.at[dx], f_recv.at[dx])
        gp_ref[:, pl.ds(pl.multiple_of((x + dx) % NX * 128, 128), 128)] = frec[dx].astype(F32)

    for copy in sends:
        copy.wait_send()
    for cond, copy in later:

        @pl.when(cond)
        def _():
            copy.wait_send()


def fused(hidden, projection, alpha, probe_pairs, amplitude, length_sq):
    pts, hid = hidden.shape
    feat = projection.shape[1]
    probes = probe_pairs.shape[1] // 2
    width = feat + AUX
    n_rows, n_cols = NZ * pts, 2 * NX * NY * pts
    size = hid // (4 * NZ)
    arrays = (hidden, projection, alpha[None, :], probe_pairs.T)
    vmem = pl.BlockSpec(memory_space=pltpu.VMEM)
    hbm = pl.BlockSpec(memory_space=pltpu.HBM)
    smem = pl.BlockSpec(memory_space=pltpu.SMEM)
    dma = pltpu.SemaphoreType.DMA
    return pl.pallas_call(
        functools.partial(kernel, probes),
        out_shape=(
            jax.ShapeDtypeStruct((pts, hid), BF),
            jax.ShapeDtypeStruct((hid // (4 * NZ), feat), F32),
        ),
        in_specs=[smem, smem, hbm, hbm, hbm, hbm],
        out_specs=(vmem, vmem),
        scratch_shapes=[
            pltpu.VMEM((n_rows, hid + AUX), BF),
            pltpu.VMEM((n_rows, feat), BF),
            pltpu.VMEM((n_cols, width), BF),
            pltpu.VMEM((n_rows, AUX), BF),
            pltpu.VMEM((n_rows, 1), F32),
            pltpu.VMEM((n_rows, feat), F32),
            pltpu.VMEM((n_rows, 128), F32),
            pltpu.VMEM((n_rows, feat), BF),
            pltpu.VMEM((4, pts, feat), BF),
            pltpu.VMEM((4, pts, feat), BF),
            pltpu.VMEM((hid, feat), F32),
            pltpu.VMEM((2, 2, 2, 2, 2 * size, feat), BF),
            pltpu.VMEM((2, 2, 2, 2 * size, feat), BF),
            pltpu.VMEM((NX, NY, 2, 2 * size, 128), BF),
            pltpu.VMEM((2, 2 * size, 128), BF),
            pltpu.VMEM((NZ, 2 * size, 128), BF),
            pltpu.VMEM((2, size, 128), BF),
            pltpu.VMEM((NX, size, 128), BF),
            dma((7 * ROW_PARTS,)),
            dma((NZ, ROW_PARTS)),
            dma((60,)),
            dma((NX, NY, 4)),
            dma((32,)),
            dma((NX, NY, 2)),
            dma((7 * PARTS,)),
            dma((2, 4, PARTS)),
            dma((1,)),
            dma((1,)),
            dma((NX, NY)),
            dma((NX, NY)),
            dma((NZ,)),
            dma((NZ,)),
            dma((NX, 2, 2)),
            dma((NX,)),
            pltpu.VMEM((hid, feat), BF),
            pltpu.VMEM((1, pts), BF),
            pltpu.VMEM((2 * probes, pts), BF),
            dma((4,)),
        ],
        compiler_params=pltpu.CompilerParams(
            collective_id=0, has_side_effects=True, vmem_limit_bytes=28 << 20
        ),
        name="fused",
    )(amplitude, length_sq, *(pltpu.with_memory_space_constraint(a, pltpu.HBM) for a in arrays))


def per_device(hidden, projection, alpha, probe_pairs, amplitude, length_sq):
    return fused(hidden, projection, alpha, probe_pairs, amplitude, length_sq)


def solution(mesh):
    placed = (P(("row", "col"), None), P(), P(("row", "col")), P(("row", "col"), None), P(), P())
    return jax.shard_map(
        per_device,
        mesh=mesh,
        in_specs=placed,
        out_specs=(P(("row", "col"), None), P("row", None)),
        check_vma=False,
    )
```
